32 devices in a mesh: section: 4 (over y, core), tensor: 2 (over x), dp: 4 (over z).
Axes of the slice: x: 2, y: 2, z: 4, core: 2. Of those that a mesh axis runs over, the one named last changes fastest.
Arguments:
- acts: bfloat16 [4, 8, 256, 2048], P('section', 'dp', 'tensor'), parts along dimension 1, may hold values from -6 to 6
- fresh: bfloat16 [8, 256, 2048], P('dp', 'tensor'), parts along dimension 0, may hold values from -6 to 6
- order: int32 [4, 2], P('section'), may hold values from 0 to 1
- ln_gain: float32 [4, 2048], P('section'), may hold values from 0.1 to 1.9
- ln_bias: float32 [4, 2048], P('section'), may hold values from -3 to 3
- wqkv: bfloat16 [4, 2048, 6144], P('section', None, 'tensor'), may hold values from -4 to 4
- wo: bfloat16 [4, 2048, 2048], P('section', 'tensor'), may hold values from -0.125 to 0.125
Outputs:
- section_out: bfloat16 [8, 4, 256, 2048], P('dp', 'section', 'tensor'), parts along dimension 0
- held: bfloat16 [4, 8, 256, 2048], P('section', 'dp', 'tensor'), parts along dimension 1
The draws below stay inside these ranges and needn't reach their ends.
There are 4 independent parts, one for each index of `dp`. The reference program is written for one: setup_inputs(seed, part) draws one part's arguments, and reference() takes and returns one part's arrays. A program takes and returns all parts, laid end to end along the dimension named above; an argument that names none is the same for every part. Nothing has to cross between parts.
All inputs are finite; a program needn't handle non-finite values.
Results may differ from the reference program's by a relative error of at most 0.017.
Values may be sent and summed in bfloat16 or wider, within the bound.
No kernel may reach another device: no remote copies, remote signals or barrier semaphores. Data moves between devices by JAX's collectives and lax.ppermute only.
A program may use at most 64 MiB of HBM per device.

```python
import jax
import jax.numpy as jnp
from jax import lax

D = 2048
HEADS = 16
HD = 128
SEQ = 256
SLOTS = 2
TICKS = 2
SECTIONS = 4
N_TENSOR = 2


def draw_wqkv(key, part):
    first = jax.random.fold_in(jax.random.fold_in(key, 11), 0)
    base = jnp.clip(jax.random.normal(first, (SECTIONS, D, HEADS, 3, HD), jnp.float32), -6.0, 6.0) * D ** (-0.5)
    return base.reshape(SECTIONS, D, HEADS * 3 * HD).astype(jnp.bfloat16)


def with_ends(values, own_key, smallest, largest):
    longest = values.shape.index(max(values.shape))
    spots = []
    for shift in (0, 1):
        where = [jax.random.randint(jax.random.fold_in(own_key, axis), (), 0, length) for axis, length in enumerate(values.shape)]
        where[longest] = (where[longest] + shift) % values.shape[longest]
        spots.append(tuple(where))
    return values.at[spots[0]].set(smallest).at[spots[1]].set(largest)


def level_of(rng, shape, cuts, low, high):
    loudness = 1.0
    for axis_at, blocks in cuts:
        steps = jax.random.uniform(jax.random.fold_in(jax.random.fold_in(rng, 6), axis_at), (blocks,), jnp.float32, low / len(cuts), high / len(cuts))
        loudness = loudness * jnp.repeat(jnp.exp(steps), shape[axis_at] // blocks).reshape((-1,) + (1,) * (len(shape) - 1 - axis_at))
    return loudness


def normal_values(rng, shape, scale, limit, cuts=(), kind=jnp.bfloat16):
    entries = jax.random.normal(rng, shape, jnp.float32) * scale
    if len(cuts) > 0:
        entries = level_of(rng, shape, cuts, -0.22, 0.18) * entries
    return jnp.clip(entries, min=-limit, max=limit).astype(kind)


def setup_inputs(seed: int = 0, part: int = 0) -> dict:
    key_list = jax.random.split(jax.random.key(seed), 8)
    own_keys = jax.random.split(jax.random.fold_in(key_list[7], part), 8)
    acts = normal_values(own_keys[0], (SECTIONS, SLOTS, SEQ, D), 1.0, 6.0, ((0, 4), (2, 2)))
    fresh = normal_values(own_keys[1], (TICKS, SEQ, D), 1.0, 6.0, ((1, 2),))
    order = with_ends(jax.random.randint(key_list[2], (SECTIONS, TICKS), 0, SLOTS), jax.random.fold_in(key_list[2], 1), 0, SLOTS - 1).astype(jnp.int32)
    ln_gain = jnp.clip(1.0 + 0.18 * jax.random.normal(key_list[3], (SECTIONS, D), jnp.float32), 0.1, 1.9)
    ln_bias = normal_values(key_list[4], (SECTIONS, D), 0.5, 3.0, ((0, 4),), jnp.float32)
    wqkv = draw_wqkv(jax.random.fold_in(key_list[7], 71), part)
    wo = normal_values(key_list[6], (SECTIONS, HEADS * HD, D), (HEADS * HD) ** -0.5, 0.125, ((0, 4), (1, 2)))
    return {"acts": acts, "fresh": fresh, "order": order, "ln_gain": ln_gain, "ln_bias": ln_bias, "wqkv": wqkv, "wo": wo}


def normed(rows, gain, bias):
    values = rows.astype(jnp.float32)
    centred = values - lax.optimization_barrier(jnp.mean(values, axis=-1, keepdims=True))
    spread = lax.optimization_barrier(jnp.mean(centred * centred, axis=-1, keepdims=True))
    return (centred * lax.rsqrt(spread + 1e-06) * gain + bias).astype(jnp.bfloat16)

def layer(inputs):
    rows, gain, bias, w_in, w_out = inputs
    normal_rows = normed(rows, gain, bias)
    qkv = jnp.dot(normal_rows, w_in, preferred_element_type=jnp.float32).astype(jnp.bfloat16)
    grid = qkv.reshape(SEQ, HEADS, 3, HD).astype(jnp.float32)
    scores = jnp.einsum('qhe,khe->hqk', grid[:, :, 0], grid[:, :, 1]) / jnp.sqrt(jnp.float32(HD))
    probs = jax.nn.softmax(scores, axis=-1).astype(jnp.bfloat16)
    attn = jnp.einsum('hqk,khe->qhe', probs.astype(jnp.float32), grid[:, :, 2]).astype(jnp.bfloat16)
    grouped = attn.reshape(SEQ, N_TENSOR, HEADS // N_TENSOR * HD).astype(jnp.float32)
    wo_grouped = w_out.reshape(N_TENSOR, HEADS // N_TENSOR * HD, D).astype(jnp.float32)
    partial_value = jnp.einsum('sgc,gcd->gsd', grouped, wo_grouped).astype(jnp.bfloat16)
    partial_value = lax.optimization_barrier(partial_value)
    total = lax.optimization_barrier(jnp.sum(partial_value.astype(jnp.float32), axis=0))
    return (rows.astype(jnp.float32) + total).astype(jnp.bfloat16)

def reference(acts, fresh, order, ln_gain, ln_bias, wqkv, wo):
    slots = acts
    outputs = []
    slot_ids = jnp.arange(SLOTS, dtype=jnp.int32)
    for tick in range(TICKS):
        chosen = order[:, tick].astype(jnp.int32)
        picked = jnp.take_along_axis(slots, chosen[:, None, None, None], axis=1)[:, 0]
        results = lax.map(layer, (picked, ln_gain, ln_bias, wqkv, wo))
        outputs.append(results)
        incoming = jnp.concatenate([fresh[tick][None], results[:-1]], axis=0)
        marks = (slot_ids[None, :] == chosen[:, None])[:, :, None, None]
        slots = jnp.where(marks, incoming[:, None], slots)
    return (jnp.stack(outputs, axis=0), slots)
```

```python
import jax
import jax.numpy as jnp
from jax import lax
from jax.sharding import PartitionSpec as P

HD = 128
TICKS = 2


def from_behind(block, axis, distance):
    devices = range(lax.axis_size(axis))
    route = [(i - distance, i) for i in devices if i - distance in devices]
    return lax.ppermute(block, axis, route)


def rotate(block, axis, shift):
    size = lax.axis_size(axis)
    return lax.ppermute(block, axis, [(i, (i + shift) % size) for i in range(size)])


def normed(rows, gain, bias):
    values = rows.astype(jnp.float32)
    centred = values - jnp.mean(values, axis=-1, keepdims=True)
    spread = jnp.mean(centred * centred, axis=-1, keepdims=True)
    return (centred * lax.rsqrt(spread + 1e-06) * gain + bias).astype(jnp.bfloat16)


def attend(queries, keys):
    local_heads = queries.shape[1] // (3 * HD)
    q = queries.reshape(queries.shape[0], local_heads, 3, HD)[:, :, 0]
    grid = keys.reshape(keys.shape[0], local_heads, 3, HD)
    scores = jnp.einsum("qhe,khe->hqk", q, grid[:, :, 1], preferred_element_type=jnp.float32)
    scores = scores / jnp.sqrt(jnp.float32(HD))
    probs = jax.nn.softmax(scores, axis=-1).astype(jnp.bfloat16)
    mixed = jnp.einsum("hqk,khe->qhe", probs, grid[:, :, 2], preferred_element_type=jnp.float32)
    return mixed.astype(jnp.bfloat16).reshape(queries.shape[0], local_heads * HD)


def layer(current, gain, bias, w_in, w_out):
    size = lax.axis_size("tensor")
    blocks = [current] + [rotate(current, "tensor", j) for j in range(1, size)]
    parts = [
        jnp.dot(normed(b, gain, bias), w_in, preferred_element_type=jnp.float32).astype(jnp.bfloat16)
        for b in blocks
    ]
    keys = jnp.concatenate(parts, axis=0)
    total = current.astype(jnp.float32)
    sums = []
    for j in list(range(1, size)) + [0]:
        mixed = attend(parts[j], keys)
        piece = jnp.dot(mixed, w_out, preferred_element_type=jnp.float32).astype(jnp.bfloat16)
        sums.append(rotate(piece, "tensor", -j) if j else piece)
    added = sum(s.astype(jnp.float32) for s in sums)
    return (total + added).astype(jnp.bfloat16)


def body(acts, fresh, order, ln_gain, ln_bias, wqkv, wo):
    first = lax.axis_index("section") == 0
    slot_ids = jnp.arange(acts.shape[1], dtype=jnp.int32)
    outputs = []
    slots = acts[0]
    for tick in range(TICKS):
        chosen = order[0, tick]
        current = lax.dynamic_index_in_dim(slots, chosen, 0, keepdims=False)
        result = layer(current, ln_gain[0], ln_bias[0], wqkv[0], wo[0])
        outputs.append(result)
        arriving = from_behind(result, "section", 1)
        arriving = jnp.where(first, fresh[tick], arriving)
        slots = jnp.where((slot_ids == chosen)[:, None, None], arriving[None], slots)
    return (jnp.stack(outputs, axis=0)[:, None], slots[None])


def solution(mesh):
    return jax.shard_map(
        body,
        mesh=mesh,
        in_specs=(
            P("section", "dp", "tensor", None),
            P("dp", "tensor", None),
            P("section", None),
            P("section", None),
            P("section", None),
            P("section", None, "tensor"),
            P("section", "tensor", None),
        ),
        out_specs=(P("dp", "section", "tensor", None), P("section", "dp", "tensor", None)),
        check_vma=False,
    )
```

```python
import functools

import jax
import jax.numpy as jnp
from jax import lax
from jax.experimental import pallas as pl
from jax.experimental.pallas import tpu as pltpu
from jax.sharding import PartitionSpec as P

HD = 128
PARTS = 2
MIB = 1 << 20
F32 = jnp.float32
BF16 = jnp.bfloat16

VMEM = pl.BlockSpec(memory_space=pltpu.VMEM)
SMEM = pl.BlockSpec(memory_space=pltpu.SMEM)
ANY = pl.BlockSpec(memory_space=pl.ANY)


def inner(shape, dtype=BF16):
    return pltpu.VMEM(tuple(shape), dtype)


def held_inside(block):
    return pltpu.with_memory_space_constraint(block, pltpu.VMEM)


def call(kernel, name, outs, out_specs, in_specs, args, flops=0, scratch=(), aliases=None, limit=16):
    return pl.pallas_call(
        kernel,
        name=name,
        out_shape=outs,
        out_specs=out_specs,
        in_specs=in_specs,
        scratch_shapes=list(scratch),
        input_output_aliases=aliases or {},
        compiler_params=pltpu.CompilerParams(vmem_limit_bytes=limit * MIB),
        cost_estimate=pl.CostEstimate(flops=max(flops, 1 << 20), bytes_accessed=1 << 16, transcendentals=0),
    )(*args)


def from_behind(block, axis):
    size = lax.axis_size(axis)
    return lax.ppermute(block, axis, [(i, i + 1) for i in range(size - 1)])


def rotate(block, axis, shift):
    size = lax.axis_size(axis)
    return lax.ppermute(block, axis, [(i, (i + shift) % size) for i in range(size)])


def pick_kernel(order, acts, current, sem):
    copy = pltpu.make_async_copy(acts.at[0, order[0, 0]], current, sem)
    copy.start()
    copy.wait()


def weights_kernel(w_in, w_out, in_inside, out_inside, sems):
    copies = []
    pieces = 4
    step = w_in.shape[1] // pieces
    for i in range(pieces):
        rows = pl.ds(i * step, step)
        copies.append(pltpu.make_async_copy(w_in.at[0, rows], in_inside.at[rows], sems.at[i]))
    copies.append(pltpu.make_async_copy(w_out.at[0], out_inside, sems.at[pieces]))
    for copy in copies:
        copy.start()
    for copy in copies:
        copy.wait()


def other_kernel(order, acts, fresh, other, sems):
    first = lax.axis_index("section") == 0
    repeated = order[0, 0] == order[0, 1]
    copy = pltpu.make_async_copy(acts.at[0, order[0, 1]], other, sems.at[0])
    copy.start()
    copy.wait()

    @pl.when(jnp.logical_and(first, repeated))
    def _():
        again = pltpu.make_async_copy(fresh.at[0], other, sems.at[1])
        again.start()
        again.wait()


def normed(rows, gain, bias):
    values = rows.astype(F32)
    centred = values - jnp.mean(values, axis=-1, keepdims=True)
    spread = jnp.mean(centred * centred, axis=-1, keepdims=True)
    return (centred * lax.rsqrt(spread + 1e-06) * gain + bias).astype(BF16)


def project(rows, weights, target, width=1024):
    for start in range(0, weights.shape[1], width):
        columns = slice(start, min(start + width, weights.shape[1]))
        target[:, columns] = jnp.dot(rows, weights[:, columns], preferred_element_type=F32).astype(BF16)


def attend(q, blocks, rows, mixed):
    heads = q.shape[1] // (3 * HD)
    for head in range(heads):
        at = [slice((head * 3 + j) * HD, (head * 3 + j + 1) * HD) for j in range(3)]
        query = q[rows, at[0]]
        keys = jnp.concatenate([b[:, at[1]] for b in blocks], axis=0)
        values = jnp.concatenate([b[:, at[2]] for b in blocks], axis=0)
        scores = lax.dot_general(query, keys, (((1,), (1,)), ((), ())), preferred_element_type=F32)
        scores = scores * (1.0 / HD**0.5)
        powers = jnp.exp(scores - jnp.max(scores, axis=-1, keepdims=True))
        probs = (powers / jnp.sum(powers, axis=-1, keepdims=True)).astype(BF16)
        out = jnp.dot(probs, values, preferred_element_type=F32)
        mixed[rows, head * HD : (head + 1) * HD] = out.astype(BF16)


def own_qkv_kernel(parts, *refs):
    chunks, (gain, bias, weights, qkv, hidden) = refs[:parts], refs[parts:]
    at = 0
    for chunk in chunks:
        rows = chunk.shape[0]
        hidden[at : at + rows] = normed(chunk[...], gain[...], bias[...])
        at += rows
    project(hidden[...], weights, qkv)


def others_kernel(parts, pieces, *refs):
    chunks = refs[:parts]
    gain, bias, w_in, w_out, mine = refs[parts : parts + 5]
    qkv = refs[parts + 5]
    outs = refs[parts + 6 : parts + 6 + pieces]
    hidden, mixed = refs[parts + 6 + pieces :]
    at = 0
    for chunk in chunks:
        rows = chunk.shape[0]
        hidden[at : at + rows] = normed(chunk[...], gain[...], bias[...])
        at += rows
    project(hidden[...], w_in, qkv)
    at = 0
    for out in outs:
        rows = slice(at, at + out.shape[0])
        attend(qkv, (mine, qkv), rows, mixed)
        project(mixed[rows], w_out, out)
        at += out.shape[0]


def own_kernel(mine, theirs, w_out, out, mixed):
    attend(mine, (mine, theirs), slice(0, mine.shape[0]), mixed)
    project(mixed[...], w_out, out)


def combine_kernel(start, *refs):
    current, own, got, result = refs[0], refs[1], refs[2:-1], refs[-1]
    rows = slice(start, start + result.shape[0])
    total = own[rows].astype(F32)
    for piece in got:
        total = total + piece[...].astype(F32)
    result[...] = (current[...].astype(F32) + total).astype(BF16)


def next_kernel(start, order, arriving, other, following):
    first = lax.axis_index("section") == 0
    take = jnp.logical_and(order[0, 0] == order[0, 1], jnp.logical_not(first))
    rows = slice(start, start + following.shape[0])
    following[...] = jnp.where(take, arriving[...], other[rows])


def held_kernel(parts, order, acts, fresh, *refs):
    arrived, held = refs[:parts], refs[parts]
    first = lax.axis_index("section") == 0
    for slot in range(acts.shape[1]):
        old, new = order[0, 0] == slot, order[0, 1] == slot
        at = 0
        for chunk in arrived:
            rows = slice(at, at + chunk.shape[0])
            value = jnp.where(first, fresh[0, rows], chunk[...])
            value = jnp.where(old, value, acts[0, slot, rows])
            held[0, slot, rows] = jnp.where(new, fresh[1, rows], value)
            at += chunk.shape[0]


def put_kernel(tick, parts, *refs):
    chunks, out, sems = refs[:parts], refs[-2], refs[-1]
    copies = []
    at = 0
    for i, chunk in enumerate(chunks):
        rows = pl.ds(at, chunk.shape[0])
        copies.append(pltpu.make_async_copy(chunk, out.at[tick, 0, rows], sems.at[i]))
        at += chunk.shape[0]
    for copy in copies:
        copy.start()
    for copy in copies:
        copy.wait()


def last_kernel(parts, order, *refs):
    chunks, out, sems = refs[:parts], refs[-2], refs[-1]
    first = lax.axis_index("section") == 0

    @pl.when(jnp.logical_not(first))
    def _():
        copies = []
        at = 0
        for i, chunk in enumerate(chunks):
            rows = pl.ds(at, chunk.shape[0])
            target = out.at[0, order[0, 1], rows]
            copies.append(pltpu.make_async_copy(chunk, target, sems.at[i]))
            at += chunk.shape[0]
        for copy in copies:
            copy.start()
        for copy in copies:
            copy.wait()


def layer(chunks, gain, bias, w_in, w_out):
    size = lax.axis_size("tensor")
    parts = len(chunks)
    rows = sum(c.shape[0] for c in chunks)
    wide, deep = w_in.shape[1], w_out.shape[0]
    width = w_in.shape[0]
    got = [held_inside(rotate(c, "tensor", j)) for j in range(1, size) for c in chunks]
    mine = call(
        functools.partial(own_qkv_kernel, parts),
        "own_qkv",
        inner((rows, wide)),
        VMEM,
        [VMEM] * (parts + 3),
        [*chunks, gain, bias, w_in],
        flops=2 * rows * width * wide,
        scratch=[inner((rows, width))],
    )
    far = (size - 1) * rows
    piece = rows // PARTS
    count = (size - 1) * PARTS
    theirs, *sends = call(
        functools.partial(others_kernel, len(got), count),
        "others",
        [inner((far, wide))] + [inner((piece, width))] * count,
        [VMEM] * (count + 1),
        [VMEM] * (len(got) + 5),
        [*got, gain, bias, w_in, w_out, mine],
        flops=2 * far * width * wide,
        scratch=[inner((far, width)), inner((far, deep))],
    )
    returned = [
        [held_inside(rotate(sends[(j - 1) * PARTS + i], "tensor", -j)) for j in range(1, size)]
        for i in range(PARTS)
    ]
    own = call(
        own_kernel,
        "own",
        inner((rows, width)),
        VMEM,
        [VMEM] * 3,
        [mine, theirs, w_out],
        flops=2 * rows * width * deep,
        scratch=[inner((rows, deep))],
    )
    return own, returned


def body(acts, fresh, order, ln_gain, ln_bias, wqkv, wo):
    rows, width = acts.shape[2:]
    piece = rows // PARTS
    ticks = fresh.shape[0]
    dma = pltpu.SemaphoreType.DMA
    current = call(pick_kernel, "pick", inner((rows, width)), VMEM, [SMEM, ANY], [order, acts], scratch=[dma])
    w_in, w_out = call(
        weights_kernel,
        "weights",
        [inner(wqkv.shape[1:]), inner(wo.shape[1:])],
        [VMEM, VMEM],
        [ANY, ANY],
        [wqkv, wo],
        scratch=[dma((5,))],
        limit=24,
        flops=1 << 30,
    )
    other = call(
        other_kernel,
        "other",
        inner((rows, width)),
        VMEM,
        [SMEM, ANY, ANY],
        [order, acts, fresh],
        scratch=[dma((2,))],
    )
    chunks = [current]
    section_out = held = None
    for tick in range(ticks):
        own, returned = layer(chunks, ln_gain, ln_bias, w_in, w_out)
        results, arrived = [], []
        for i in range(PARTS):
            if len(chunks) == 1:
                source, spec = chunks[0], None
            else:
                source = chunks[i]
            whole = len(chunks) == 1

            def combine(*refs, i=i, whole=whole):
                start = i * piece
                here = refs[0].at[pl.ds(start, piece)] if whole else refs[0]
                combine_kernel(start, here, *refs[1:])

            result = call(
                combine,
                "combine",
                inner((piece, width)),
                VMEM,
                [VMEM] * (2 + len(returned[i])),
                [source, own, *returned[i]],
            )
            results.append(result)
            arrived.append(held_inside(from_behind(result, "section")))
        if tick == 0:
            section_out = call(
                functools.partial(put_kernel, tick, PARTS),
                "put",
                jax.ShapeDtypeStruct((ticks, 1, rows, width), BF16),
                ANY,
                [VMEM] * PARTS,
                results,
                scratch=[dma((PARTS,))],
            )
            chunks = [
                call(
                    functools.partial(next_kernel, i * piece),
                    "next",
                    inner((piece, width)),
                    VMEM,
                    [SMEM, VMEM, VMEM],
                    [order, arrived[i], other],
                )
                for i in range(PARTS)
            ]
            held = call(
                functools.partial(held_kernel, PARTS),
                "held",
                jax.ShapeDtypeStruct(acts.shape, BF16),
                VMEM,
                [SMEM, VMEM, VMEM] + [VMEM] * PARTS,
                [order, acts, fresh, *arrived],
            )
        else:
            section_out = call(
                functools.partial(put_kernel, tick, PARTS),
                "put",
                jax.ShapeDtypeStruct((ticks, 1, rows, width), BF16),
                ANY,
                [VMEM] * PARTS + [ANY],
                [*results, section_out],
                scratch=[dma((PARTS,))],
                aliases={PARTS: 0},
            )
            held = call(
                functools.partial(last_kernel, PARTS),
                "last",
                jax.ShapeDtypeStruct(acts.shape, BF16),
                ANY,
                [SMEM] + [VMEM] * PARTS + [ANY],
                [order, *arrived, held],
                scratch=[dma((PARTS,))],
                aliases={PARTS + 1: 0},
            )
    return section_out, held


def solution(mesh):
    return jax.shard_map(
        body,
        mesh=mesh,
        in_specs=(
            P("section", "dp", "tensor", None),
            P("dp", "tensor", None),
            P("section", None),
            P("section", None),
            P("section", None),
            P("section", None, "tensor"),
            P("section", "tensor", None),
        ),
        out_specs=(P("dp", "section", "tensor", None), P("section", "dp", "tensor", None)),
        check_vma=False,
    )
```

```python
import functools

import jax
import jax.numpy as jnp
from jax import lax
from jax.experimental import pallas as pl
from jax.experimental.pallas import tpu as pltpu
from jax.sharding import PartitionSpec as P

HD = 128
PARTS = 2
MIB = 1 << 20
F32 = jnp.float32
BF16 = jnp.bfloat16

VMEM = pl.BlockSpec(memory_space=pltpu.VMEM)
SMEM = pl.BlockSpec(memory_space=pltpu.SMEM)
ANY = pl.BlockSpec(memory_space=pl.ANY)


def inner(shape, dtype=BF16):
    return pltpu.VMEM(tuple(shape), dtype)


def held_inside(block):
    return pltpu.with_memory_space_constraint(block, pltpu.VMEM)


def outside(block):
    return pltpu.with_memory_space_constraint(block, pltpu.HBM)


def after(kernel, count):
    return lambda *refs: kernel(*refs[count:])


def call(kernel, name, outs, out_specs, in_specs, args, flops=0, scratch=(), aliases=None, limit=16, wait=()):
    if wait:
        kernel = after(kernel, len(wait))
        in_specs, args = [ANY] * len(wait) + in_specs, [*wait, *args]
        aliases = {k + len(wait): v for k, v in (aliases or {}).items()}
    return pl.pallas_call(
        kernel,
        name=name,
        out_shape=outs,
        out_specs=out_specs,
        in_specs=in_specs,
        scratch_shapes=list(scratch),
        input_output_aliases=aliases or {},
        compiler_params=pltpu.CompilerParams(vmem_limit_bytes=limit * MIB),
        cost_estimate=pl.CostEstimate(flops=max(flops, 1 << 20), bytes_accessed=1 << 16, transcendentals=0),
    )(*args)


def from_behind(block, axis):
    size = lax.axis_size(axis)
    return lax.ppermute(block, axis, [(i, i + 1) for i in range(size - 1)])


def rotate(block, axis, shift):
    size = lax.axis_size(axis)
    return lax.ppermute(block, axis, [(i, (i + shift) % size) for i in range(size)])


def pick_kernel(order, acts, current, kept, slots, sems):
    number = pltpu.make_async_copy(order, kept, sems.at[0])
    blocks = pltpu.make_async_copy(acts.at[0], slots, sems.at[1])
    number.start()
    blocks.start()
    number.wait()
    blocks.wait()
    current[...] = slots[kept[0, 0]]


def weights_kernel(w_in, w_out, in_inside, out_inside, sems):
    copies = []
    pieces = 4
    step = w_in.shape[1] // pieces
    for i in range(pieces):
        rows = pl.ds(i * step, step)
        copies.append(pltpu.make_async_copy(w_in.at[0, rows], in_inside.at[rows], sems.at[i]))
    copies.append(pltpu.make_async_copy(w_out.at[0], out_inside, sems.at[pieces]))
    for copy in copies:
        copy.start()
    for copy in copies:
        copy.wait()


def other_kernel(order, acts, fresh, other, sems):
    first = lax.axis_index("section") == 0
    repeated = order[0, 0] == order[0, 1]
    copy = pltpu.make_async_copy(acts.at[0, order[0, 1]], other, sems.at[0])
    copy.start()
    copy.wait()

    @pl.when(jnp.logical_and(first, repeated))
    def _():
        again = pltpu.make_async_copy(fresh.at[0], other, sems.at[1])
        again.start()
        again.wait()


def normed(rows, gain, bias):
    values = rows.astype(F32)
    centred = values - jnp.mean(values, axis=-1, keepdims=True)
    spread = jnp.mean(centred * centred, axis=-1, keepdims=True)
    return (centred * lax.rsqrt(spread + 1e-06) * gain + bias).astype(BF16)


def project(rows, weights, *targets, width=1024):
    for start in range(0, weights.shape[1], width):
        columns = slice(start, min(start + width, weights.shape[1]))
        value = jnp.dot(rows, weights[:, columns], preferred_element_type=F32).astype(BF16)
        at = 0
        for target in targets:
            target[:, columns] = value[at : at + target.shape[0]]
            at += target.shape[0]


def attend(q, blocks, rows, mixed):
    heads = q.shape[1] // (3 * HD)
    for head in range(heads):
        at = [slice((head * 3 + j) * HD, (head * 3 + j + 1) * HD) for j in range(3)]
        query = q[rows, at[0]]
        keys = jnp.concatenate([b[:, at[1]] for b in blocks], axis=0)
        values = jnp.concatenate([b[:, at[2]] for b in blocks], axis=0)
        scores = lax.dot_general(query, keys, (((1,), (1,)), ((), ())), preferred_element_type=F32)
        scores = scores * (1.0 / HD**0.5)
        powers = jnp.exp(scores - jnp.max(scores, axis=-1, keepdims=True))
        probs = (powers / jnp.sum(powers, axis=-1, keepdims=True)).astype(BF16)
        out = jnp.dot(probs, values, preferred_element_type=F32)
        mixed[rows, head * HD : (head + 1) * HD] = out.astype(BF16)


def own_qkv_kernel(parts, *refs):
    chunks, (gain, bias, weights, qkv, hidden) = refs[:parts], refs[parts:]
    at = 0
    for chunk in chunks:
        rows = chunk.shape[0]
        hidden[at : at + rows] = normed(chunk[...], gain[...], bias[...])
        at += rows
    project(hidden[...], weights, qkv)


def others_kernel(parts, pieces, *refs):
    chunks = refs[:parts]
    gain, bias, w_in, w_out, mine = refs[parts : parts + 5]
    qkv = refs[parts + 5]
    outs = refs[parts + 6 : parts + 6 + pieces]
    hidden, mixed = refs[parts + 6 + pieces :]
    at = 0
    for chunk in chunks:
        rows = chunk.shape[0]
        hidden[at : at + rows] = normed(chunk[...], gain[...], bias[...])
        at += rows
    project(hidden[...], w_in, qkv)
    attend(qkv, (mine, qkv), slice(0, at), mixed)
    project(mixed[...], w_out, *outs)


def own_kernel(mine, theirs, w_out, out, mixed):
    attend(mine, (mine, theirs), slice(0, mine.shape[0]), mixed)
    project(mixed[...], w_out, out)


def combine_kernel(start, *refs):
    current, own, got, result = refs[0], refs[1], refs[2:-1], refs[-1]
    rows = slice(start, start + result.shape[0])
    total = own[rows].astype(F32)
    for piece in got:
        total = total + piece[...].astype(F32)
    result[...] = (current[...].astype(F32) + total).astype(BF16)


def next_kernel(start, order, arriving, other, following):
    first = lax.axis_index("section") == 0
    take = jnp.logical_and(order[0, 0] == order[0, 1], jnp.logical_not(first))
    rows = slice(start, start + following.shape[0])
    following[...] = jnp.where(take, arriving[...], other[rows])


def held_kernel(parts, order, acts, fresh, *refs):
    arrived, held = refs[:parts], refs[parts]
    first = lax.axis_index("section") == 0
    for slot in range(acts.shape[1]):
        old, new = order[0, 0] == slot, order[0, 1] == slot
        at = 0
        for chunk in arrived:
            rows = slice(at, at + chunk.shape[0])
            value = jnp.where(first, fresh[0, rows], chunk[...])
            value = jnp.where(old, value, acts[0, slot, rows])
            held[0, slot, rows] = jnp.where(new, fresh[1, rows], value)
            at += chunk.shape[0]


def put_kernel(tick, parts, *refs):
    chunks, out, sems = refs[:parts], refs[-2], refs[-1]
    copies = []
    at = 0
    for i, chunk in enumerate(chunks):
        rows = pl.ds(at, chunk.shape[0])
        copies.append(pltpu.make_async_copy(chunk, out.at[tick, 0, rows], sems.at[i]))
        at += chunk.shape[0]
    for copy in copies:
        copy.start()
    for copy in copies:
        copy.wait()


def last_kernel(parts, order, *refs):
    chunks, out, sems = refs[:parts], refs[-2], refs[-1]
    first = lax.axis_index("section") == 0

    @pl.when(jnp.logical_not(first))
    def _():
        copies = []
        at = 0
        for i, chunk in enumerate(chunks):
            rows = pl.ds(at, chunk.shape[0])
            target = out.at[0, order[0, 1], rows]
            copies.append(pltpu.make_async_copy(chunk, target, sems.at[i]))
            at += chunk.shape[0]
        for copy in copies:
            copy.start()
        for copy in copies:
            copy.wait()


def cuts(rows):
    units = rows // 16
    parts = min(PARTS, units)
    sizes = [(units // parts + (i < units % parts)) * 16 for i in range(parts)]
    return [(sum(sizes[:i]), size) for i, size in enumerate(sizes)]


def layer(chunks, gain, bias, w_in, w_out, early=(), late=None):
    size = lax.axis_size("tensor")
    parts = len(chunks)
    rows = sum(c.shape[0] for c in chunks)
    wide, deep = w_in.shape[1], w_out.shape[0]
    width = w_in.shape[0]
    got = [held_inside(rotate(c, "tensor", j)) for j in range(1, size) for c in chunks]
    mine = call(
        functools.partial(own_qkv_kernel, parts),
        "own_qkv",
        inner((rows, wide)),
        VMEM,
        [VMEM] * (parts + 3),
        [*chunks, gain, bias, w_in],
        flops=2 * rows * width * wide,
        scratch=[inner((rows, width))],
    )
    far = (size - 1) * rows
    pieces = cuts(rows)
    count = (size - 1) * len(pieces)
    done = late(mine) if late else []
    theirs, *sends = call(
        functools.partial(others_kernel, len(got), count),
        "others",
        [inner((far, wide))] + [inner((n, width)) for _ in range(size - 1) for _, n in pieces],
        [VMEM] * (count + 1),
        [VMEM] * (len(got) + 5),
        [*got, gain, bias, w_in, w_out, mine],
        flops=2 * far * width * wide,
        scratch=[inner((far, width)), inner((far, deep))],
        wait=[*early, *done],
    )
    returned = [
        [held_inside(rotate(sends[(j - 1) * len(pieces) + i], "tensor", -j)) for j in range(1, size)]
        for i in range(len(pieces))
    ]
    own = call(
        own_kernel,
        "own",
        inner((rows, width)),
        VMEM,
        [VMEM] * 3,
        [mine, theirs, w_out],
        flops=2 * rows * width * deep,
        scratch=[inner((rows, deep))],
    )
    return own, returned, done


def body(acts, fresh, order, ln_gain, ln_bias, wqkv, wo):
    rows, width = acts.shape[2:]
    piece = rows // PARTS
    ticks = fresh.shape[0]
    dma = pltpu.SemaphoreType.DMA
    acts, fresh, order, wqkv, wo = map(outside, (acts, fresh, order, wqkv, wo))
    current, order = call(
        pick_kernel,
        "pick",
        [inner((rows, width)), pltpu.SMEM(order.shape, order.dtype)],
        [VMEM, SMEM],
        [ANY, ANY],
        [order, acts],
        scratch=[inner(acts.shape[1:]), dma((2,))],
    )
    w_in, w_out = call(
        weights_kernel,
        "weights",
        [inner(wqkv.shape[1:]), inner(wo.shape[1:])],
        [VMEM, VMEM],
        [ANY, ANY],
        [wqkv, wo],
        scratch=[dma((5,))],
        limit=24,
        flops=1 << 30,
    )
    other = call(
        other_kernel,
        "other",
        inner((rows, width)),
        VMEM,
        [SMEM, ANY, ANY],
        [order, acts, fresh],
        scratch=[dma((2,))],
    )
    chunks = [current]
    pieces = cuts(rows)
    parts = len(pieces)
    section_out = held = late = None
    early = [other]
    for tick in range(ticks):
        own, returned, done = layer(chunks, ln_gain, ln_bias, w_in, w_out, early, late)
        results, arrived = [], []
        for i, (start, size) in enumerate(pieces):

            def combine(*refs, start=start, size=size, whole=len(chunks) == 1):
                here = refs[0].at[pl.ds(start, size)] if whole else refs[0]
                combine_kernel(start, here, *refs[1:])

            result = call(
                combine,
                "combine",
                inner((size, width)),
                VMEM,
                [VMEM] * (2 + len(returned[i])),
                [chunks[min(i, len(chunks) - 1)], own, *returned[i]],
            )
            results.append(result)
            arrived.append(held_inside(from_behind(result, "section")))
        if tick == 0:
            chunks = [
                call(
                    functools.partial(next_kernel, start),
                    "next",
                    inner((size, width)),
                    VMEM,
                    [SMEM, VMEM, VMEM],
                    [order, arrived[i], other],
                )
                for i, (start, size) in enumerate(pieces)
            ]
            early = []

            def late(mine, results=results, arrived=arrived):
                put = call(
                    functools.partial(put_kernel, 0, parts),
                    "put",
                    pltpu.HBM((ticks, 1, rows, width), BF16),
                    ANY,
                    [VMEM] * parts,
                    results,
                    scratch=[dma((parts,))],
                    wait=[mine],
                )
                held = call(
                    functools.partial(held_kernel, parts),
                    "held",
                    pltpu.HBM(acts.shape, BF16),
                    VMEM,
                    [SMEM, VMEM, VMEM] + [VMEM] * parts,
                    [order, acts, fresh, *arrived],
                    wait=[mine],
                )
                return [outside(put), outside(held)]

        else:
            section_out, held = done
            section_out = call(
                functools.partial(put_kernel, tick, parts),
                "put",
                jax.ShapeDtypeStruct((ticks, 1, rows, width), BF16),
                ANY,
                [VMEM] * parts + [ANY],
                [*results, section_out],
                scratch=[dma((parts,))],
                aliases={parts: 0},
            )
            held = call(
                functools.partial(last_kernel, parts),
                "last",
                jax.ShapeDtypeStruct(acts.shape, BF16),
                ANY,
                [SMEM] + [VMEM] * parts + [ANY],
                [order, *arrived, held],
                scratch=[dma((parts,))],
                aliases={parts + 1: 0},
            )
    return section_out, held


def solution(mesh):
    return jax.shard_map(
        body,
        mesh=mesh,
        in_specs=(
            P("section", "dp", "tensor", None),
            P("dp", "tensor", None),
            P("section", None),
            P("section", None),
            P("section", None),
            P("section", None, "tensor"),
            P("section", "tensor", None),
        ),
        out_specs=(P("dp", "section", "tensor", None), P("section", "dp", "tensor", None)),
        check_vma=False,
    )
```

```python
import functools

import jax
import jax.numpy as jnp
from jax import lax
from jax.experimental import pallas as pl
from jax.experimental.pallas import tpu as pltpu
from jax.sharding import PartitionSpec as P


HD = 128
PARTS = 2
MIB = 1 << 20
F32 = jnp.float32
BF16 = jnp.bfloat16

VMEM = pl.BlockSpec(memory_space=pltpu.VMEM)
SMEM = pl.BlockSpec(memory_space=pltpu.SMEM)
ANY = pl.BlockSpec(memory_space=pl.ANY)


def inner(shape, dtype=BF16):
    return pltpu.VMEM(tuple(shape), dtype)


def held_inside(block):
    return pltpu.with_memory_space_constraint(block, pltpu.VMEM)


def outside(block):
    return pltpu.with_memory_space_constraint(block, pltpu.HBM)


def after(kernel, count):
    return lambda *refs: kernel(*refs[count:])


def call(kernel, outs, out_specs, in_specs, args, flops=0, scratch=(), aliases=None, limit=16, wait=()):
    if wait:
        kernel = after(kernel, len(wait))
        in_specs, args = [ANY] * len(wait) + in_specs, [*wait, *args]
        aliases = {k + len(wait): v for k, v in (aliases or {}).items()}
    return pl.pallas_call(
        kernel,
        out_shape=outs,
        out_specs=out_specs,
        in_specs=in_specs,
        scratch_shapes=list(scratch),
        input_output_aliases=aliases or {},
        compiler_params=pltpu.CompilerParams(vmem_limit_bytes=limit * MIB),
        cost_estimate=pl.CostEstimate(flops=max(flops, 1 << 20), bytes_accessed=1 << 16, transcendentals=0),
    )(*args)


def from_behind(block, axis):
    size = lax.axis_size(axis)
    return lax.ppermute(block, axis, [(i, i + 1) for i in range(size - 1)])


def rotate(block, shift, sections):
    size = lax.axis_size("tensor")
    route = [(s * size + i, s * size + (i + shift) % size) for s in sections for i in range(size)]
    return held_inside(lax.ppermute(block, ("section", "tensor"), route))


def pick_kernel(order, acts, current, kept, slots, sems):
    number = pltpu.make_async_copy(order, kept, sems.at[0])
    blocks = pltpu.make_async_copy(acts.at[0], slots, sems.at[1])
    number.start()
    blocks.start()
    number.wait()
    blocks.wait()
    current[...] = slots[kept[0, 0]]


def weights_kernel(w_in, w_out, in_inside, out_inside, sems):
    copies = []
    pieces = 4
    step = w_in.shape[1] // pieces
    for i in range(pieces):
        rows = pl.ds(i * step, step)
        copies.append(pltpu.make_async_copy(w_in.at[0, rows], in_inside.at[rows], sems.at[i]))
    copies.append(pltpu.make_async_copy(w_out.at[0], out_inside, sems.at[pieces]))
    for copy in copies:
        copy.start()
    for copy in copies:
        copy.wait()


def other_kernel(order, acts, fresh, other, sems):
    first = lax.axis_index("section") == 0
    repeated = order[0, 0] == order[0, 1]
    copy = pltpu.make_async_copy(acts.at[0, order[0, 1]], other, sems.at[0])
    copy.start()
    copy.wait()

    @pl.when(jnp.logical_and(first, repeated))
    def _():
        again = pltpu.make_async_copy(fresh.at[0], other, sems.at[1])
        again.start()
        again.wait()


def normed(rows, gain, bias):
    values = rows.astype(F32)
    centred = values - jnp.mean(values, axis=-1, keepdims=True)
    spread = jnp.mean(centred * centred, axis=-1, keepdims=True)
    return (centred * lax.rsqrt(spread + 1e-06) * gain + bias).astype(BF16)


def project(rows, weights, *targets, width=1024):
    for start in range(0, weights.shape[1], width):
        columns = slice(start, min(start + width, weights.shape[1]))
        value = jnp.dot(rows, weights[:, columns], preferred_element_type=F32).astype(BF16)
        at = 0
        for target in targets:
            target[:, columns] = value[at : at + target.shape[0]]
            at += target.shape[0]


def attend(q, blocks, rows, mixed):
    heads = q.shape[1] // (3 * HD)
    for head in range(heads):
        at = [slice((head * 3 + j) * HD, (head * 3 + j + 1) * HD) for j in range(3)]
        query = q[rows, at[0]]
        keys = jnp.concatenate([b[:, at[1]] for b in blocks], axis=0)
        values = jnp.concatenate([b[:, at[2]] for b in blocks], axis=0)
        scores = lax.dot_general(query, keys, (((1,), (1,)), ((), ())), preferred_element_type=F32)
        scores = scores * (1.0 / HD**0.5)
        powers = jnp.exp(scores - jnp.max(scores, axis=-1, keepdims=True))
        probs = (powers / jnp.sum(powers, axis=-1, keepdims=True)).astype(BF16)
        out = jnp.dot(probs, values, preferred_element_type=F32)
        mixed[rows, head * HD : (head + 1) * HD] = out.astype(BF16)


def own_qkv_kernel(parts, *refs):
    chunks, (gain, bias, weights, qkv, hidden) = refs[:parts], refs[parts:]
    at = 0
    for chunk in chunks:
        rows = chunk.shape[0]
        hidden[at : at + rows] = normed(chunk[...], gain[...], bias[...])
        at += rows
    project(hidden[...], weights, qkv)


def others_kernel(parts, pieces, spare, *refs):
    chunks, alone, refs = refs[:parts], refs[parts : parts + spare], refs[:parts] + refs[parts + spare :]
    first = lax.axis_index("section") == 0
    gain, bias, w_in, w_out, mine = refs[parts : parts + 5]
    qkv = refs[parts + 5]
    outs = refs[parts + 6 : parts + 6 + pieces]
    hidden, mixed = refs[parts + 6 + pieces :]
    at = 0
    for chunk in chunks:
        rows = chunk.shape[0]
        value = chunk[...]
        if alone:
            start = at % alone[0].shape[0]
            value = jnp.where(first, alone[at // alone[0].shape[0]][start : start + rows], value)
        hidden[at : at + rows] = normed(value, gain[...], bias[...])
        at += rows
    project(hidden[...], w_in, qkv)
    attend(qkv, (mine, qkv), slice(0, at), mixed)
    project(mixed[...], w_out, *outs)


def own_kernel(mine, theirs, w_out, out, mixed):
    attend(mine, (mine, theirs), slice(0, mine.shape[0]), mixed)
    project(mixed[...], w_out, out)


def combine_kernel(start, *refs):
    current, own, got, result = refs[0], refs[1], refs[2:-1], refs[-1]
    rows = slice(start, start + result.shape[0])
    total = own[rows].astype(F32)
    for piece in got:
        total = total + piece[...].astype(F32)
    result[...] = (current[...].astype(F32) + total).astype(BF16)


def next_kernel(start, order, arriving, other, following):
    first = lax.axis_index("section") == 0
    take = jnp.logical_and(order[0, 0] == order[0, 1], jnp.logical_not(first))
    rows = slice(start, start + following.shape[0])
    following[...] = jnp.where(take, arriving[...], other[rows])


def held_kernel(parts, order, acts, fresh, *refs):
    arrived, held = refs[:parts], refs[parts]
    first = lax.axis_index("section") == 0
    for slot in range(acts.shape[1]):
        old, new = order[0, 0] == slot, order[0, 1] == slot
        at = 0
        for chunk in arrived:
            rows = slice(at, at + chunk.shape[0])
            value = jnp.where(first, fresh[0, rows], chunk[...])
            value = jnp.where(old, value, acts[0, slot, rows])
            held[0, slot, rows] = jnp.where(new, fresh[1, rows], value)
            at += chunk.shape[0]


def put_kernel(tick, parts, *refs):
    chunks, out, sems = refs[:parts], refs[-2], refs[-1]
    copies = []
    at = 0
    for i, chunk in enumerate(chunks):
        rows = pl.ds(at, chunk.shape[0])
        copies.append(pltpu.make_async_copy(chunk, out.at[tick, 0, rows], sems.at[i]))
        at += chunk.shape[0]
    for copy in copies:
        copy.start()
    for copy in copies:
        copy.wait()


def last_kernel(parts, order, *refs):
    chunks, out, sems = refs[:parts], refs[-2], refs[-1]
    first = lax.axis_index("section") == 0

    @pl.when(jnp.logical_not(first))
    def _():
        copies = []
        at = 0
        for i, chunk in enumerate(chunks):
            rows = pl.ds(at, chunk.shape[0])
            target = out.at[0, order[0, 1], rows]
            copies.append(pltpu.make_async_copy(chunk, target, sems.at[i]))
            at += chunk.shape[0]
        for copy in copies:
            copy.start()
        for copy in copies:
            copy.wait()


def cuts(rows):
    units = rows // 16
    parts = min(PARTS, units)
    sizes = [(units // parts + (i < units % parts)) * 16 for i in range(parts)]
    return [(sum(sizes[:i]), size) for i, size in enumerate(sizes)]


def layer(chunks, gain, bias, w_in, w_out, alone=(), early=()):
    size = lax.axis_size("tensor")
    sections = range(lax.axis_size("section"))
    parts = len(chunks)
    rows = sum(c.shape[0] for c in chunks)
    wide, deep = w_in.shape[1], w_out.shape[0]
    width = w_in.shape[0]
    got = [rotate(c, j, sections[1:] if alone else sections) for j in range(1, size) for c in chunks]
    mine = call(
        functools.partial(own_qkv_kernel, parts),
        inner((rows, wide)),
        VMEM,
        [VMEM] * (parts + 3),
        [*chunks, gain, bias, w_in],
        flops=2 * rows * width * wide,
        scratch=[inner((rows, width))],
    )
    far = (size - 1) * rows
    pieces = cuts(rows)
    count = (size - 1) * len(pieces)
    theirs, *sends = call(
        functools.partial(others_kernel, len(got), count, len(alone)),
        [inner((far, wide))] + [inner((n, width)) for _ in range(size - 1) for _, n in pieces],
        [VMEM] * (count + 1),
        [VMEM] * (len(got) + len(alone) + 5),
        [*got, *alone, gain, bias, w_in, w_out, mine],
        flops=2 * far * width * wide,
        scratch=[inner((far, width)), inner((far, deep))],
        wait=early,
    )
    returned = [
        [rotate(sends[(j - 1) * len(pieces) + i], -j, sections) for j in range(1, size)]
        for i in range(len(pieces))
    ]
    own = call(
        own_kernel,
        inner((rows, width)),
        VMEM,
        [VMEM] * 3,
        [mine, theirs, w_out],
        flops=2 * rows * width * deep,
        scratch=[inner((rows, deep))],
    )
    return own, returned


def body(acts, fresh, order, ln_gain, ln_bias, wqkv, wo):
    rows, width = acts.shape[2:]
    ticks = fresh.shape[0]
    dma = pltpu.SemaphoreType.DMA
    acts, fresh, order, wqkv, wo = map(outside, (acts, fresh, order, wqkv, wo))
    current, order = call(
        pick_kernel,
        [inner((rows, width)), pltpu.SMEM(order.shape, order.dtype)],
        [VMEM, SMEM],
        [ANY, ANY],
        [order, acts],
        scratch=[inner(acts.shape[1:]), dma((2,))],
    )
    other = call(
        other_kernel,
        inner((rows, width)),
        VMEM,
        [SMEM, ANY, ANY],
        [order, acts, fresh],
        scratch=[dma((2,))],
    )
    alone = [rotate(other, j, [0]) for j in range(1, lax.axis_size("tensor"))]
    w_in, w_out = call(
        weights_kernel,
        [inner(wqkv.shape[1:]), inner(wo.shape[1:])],
        [VMEM, VMEM],
        [ANY, ANY],
        [wqkv, wo],
        scratch=[dma((5,))],
        limit=24,
        flops=1 << 30,
    )
    chunks = [current]
    pieces = cuts(rows)
    parts = len(pieces)
    section_out = held = None
    for tick in range(ticks):
        own, returned = layer(chunks, ln_gain, ln_bias, w_in, w_out, alone if tick else ())
        ready = []
        if tick:
            section_out = call(
                functools.partial(put_kernel, 0, parts),
                pltpu.HBM((ticks, 1, rows, width), BF16),
                ANY,
                [VMEM] * parts,
                results,
                scratch=[dma((parts,))],
                wait=[own],
            )
            held = call(
                functools.partial(held_kernel, parts),
                pltpu.HBM(acts.shape, BF16),
                VMEM,
                [SMEM, VMEM, VMEM] + [VMEM] * parts,
                [order, acts, fresh, *arrived],
                wait=[own],
            )
            section_out, held = outside(section_out), outside(held)
            ready = [section_out, held]
        results, arrived = [], []
        for i, (start, size) in enumerate(pieces):

            def combine(*refs, start=start, size=size, whole=len(chunks) == 1):
                here = refs[0].at[pl.ds(start, size)] if whole else refs[0]
                combine_kernel(start, here, *refs[1:])

            result = call(
                combine,
                inner((size, width)),
                VMEM,
                [VMEM] * (2 + len(returned[i])),
                [chunks[min(i, len(chunks) - 1)], own, *returned[i]],
                wait=ready,
            )
            results.append(result)
            arrived.append(held_inside(from_behind(result, "section")))
        if tick == 0:
            chunks = [
                call(
                    functools.partial(next_kernel, start),
                    inner((size, width)),
                    VMEM,
                    [SMEM, VMEM, VMEM],
                    [order, arrived[i], other],
                )
                for i, (start, size) in enumerate(pieces)
            ]
    section_out = call(
        functools.partial(put_kernel, ticks - 1, parts),
        jax.ShapeDtypeStruct((ticks, 1, rows, width), BF16),
        ANY,
        [VMEM] * parts + [ANY],
        [*results, section_out],
        scratch=[dma((parts,))],
        aliases={parts: 0},
    )
    held = call(
        functools.partial(last_kernel, parts),
        jax.ShapeDtypeStruct(acts.shape, BF16),
        ANY,
        [SMEM] + [VMEM] * parts + [ANY],
        [order, *arrived, held],
        scratch=[dma((parts,))],
        aliases={parts + 1: 0},
    )
    return section_out, held


def solution(mesh):
    return jax.shard_map(
        body,
        mesh=mesh,
        in_specs=(
            P("section", "dp", "tensor", None),
            P("dp", "tensor", None),
            P("section", None),
            P("section", None),
            P("section", None),
            P("section", None, "tensor"),
            P("section", "tensor", None),
        ),
        out_specs=(P("dp", "section", "tensor", None), P("section", "dp", "tensor", None)),
        check_vma=False,
    )
```

```python
import functools

import jax
import jax.numpy as jnp
from jax import lax
from jax.experimental import pallas as pl
from jax.experimental.pallas import tpu as pltpu
from jax.sharding import PartitionSpec as P


HD = 128
SHARES = ((1, 1), (2, 1, 1))
MIB = 1 << 20
F32 = jnp.float32
BF16 = jnp.bfloat16

VMEM = pl.BlockSpec(memory_space=pltpu.VMEM)
SMEM = pl.BlockSpec(memory_space=pltpu.SMEM)
ANY = pl.BlockSpec(memory_space=pl.ANY)


def inner(shape, dtype=BF16):
    return pltpu.VMEM(tuple(shape), dtype)


def held_inside(block):
    return pltpu.with_memory_space_constraint(block, pltpu.VMEM)


def outside(block):
    return pltpu.with_memory_space_constraint(block, pltpu.HBM)


def after(kernel, count):
    return lambda *refs: kernel(*refs[count:])


def call(kernel, outs, out_specs, in_specs, args, flops=0, scratch=(), aliases=None, limit=16, wait=()):
    if wait:
        kernel = after(kernel, len(wait))
        in_specs, args = [ANY] * len(wait) + in_specs, [*wait, *args]
        aliases = {k + len(wait): v for k, v in (aliases or {}).items()}
    return pl.pallas_call(
        kernel,
        out_shape=outs,
        out_specs=out_specs,
        in_specs=in_specs,
        scratch_shapes=list(scratch),
        input_output_aliases=aliases or {},
        compiler_params=pltpu.CompilerParams(vmem_limit_bytes=limit * MIB),
        cost_estimate=pl.CostEstimate(flops=max(flops, 1 << 20), bytes_accessed=1 << 16, transcendentals=0),
    )(*args)


def from_behind(block, axis):
    size = lax.axis_size(axis)
    return lax.ppermute(block, axis, [(i, (i + 1) % size) for i in range(size)])


def rotate(block, shift, sections, rest=False):
    names = ("section", "tensor", "dp")
    count, size, groups = map(lax.axis_size, names)
    route = []
    for s in range(count):
        for i in range(size):
            for d in range(groups):
                here = (s * size + i) * groups + d
                if s in sections:
                    route.append((here, (s * size + (i + shift) % size) * groups + d))
                elif rest and d ^ 1 < groups:
                    route.append((here, here - d + (d ^ 1)))
    return held_inside(lax.ppermute(block, names, route))


def pick_kernel(order, acts, current, kept, slots, sems):
    number = pltpu.make_async_copy(order, kept, sems.at[0])
    blocks = pltpu.make_async_copy(acts.at[0], slots, sems.at[1])
    number.start()
    blocks.start()
    number.wait()
    blocks.wait()
    current[...] = slots[kept[0, 0]]


def weights_kernel(w_in, w_out, in_inside, out_inside, sems):
    copies = []
    pieces = 4
    step = w_in.shape[1] // pieces
    for i in range(pieces):
        rows = pl.ds(i * step, step)
        copies.append(pltpu.make_async_copy(w_in.at[0, rows], in_inside.at[rows], sems.at[i]))
    copies.append(pltpu.make_async_copy(w_out.at[0], out_inside, sems.at[pieces]))
    for copy in copies:
        copy.start()
    for copy in copies:
        copy.wait()


def other_kernel(order, acts, fresh, other, sems):
    first = lax.axis_index("section") == 0
    repeated = order[0, 0] == order[0, 1]
    copy = pltpu.make_async_copy(acts.at[0, order[0, 1]], other, sems.at[0])
    copy.start()
    copy.wait()

    @pl.when(jnp.logical_and(first, repeated))
    def _():
        again = pltpu.make_async_copy(fresh.at[0], other, sems.at[1])
        again.start()
        again.wait()


def normed(rows, gain, bias):
    values = rows.astype(F32)
    centred = values - jnp.mean(values, axis=-1, keepdims=True)
    spread = jnp.mean(centred * centred, axis=-1, keepdims=True)
    return (centred * lax.rsqrt(spread + 1e-06) * gain + bias).astype(BF16)


def project(rows, weights, *targets, width=1024):
    for start in range(0, weights.shape[1], width):
        columns = slice(start, min(start + width, weights.shape[1]))
        value = jnp.dot(rows, weights[:, columns], preferred_element_type=F32).astype(BF16)
        at = 0
        for target in targets:
            target[:, columns] = value[at : at + target.shape[0]]
            at += target.shape[0]


def attend(q, blocks, rows, mixed):
    heads = q.shape[1] // (3 * HD)
    for head in range(heads):
        at = [slice((head * 3 + j) * HD, (head * 3 + j + 1) * HD) for j in range(3)]
        query = q[rows, at[0]]
        keys = jnp.concatenate([b[:, at[1]] for b in blocks], axis=0)
        values = jnp.concatenate([b[:, at[2]] for b in blocks], axis=0)
        scores = lax.dot_general(query, keys, (((1,), (1,)), ((), ())), preferred_element_type=F32)
        scores = scores * (1.0 / HD**0.5)
        powers = jnp.exp(scores - jnp.max(scores, axis=-1, keepdims=True))
        probs = (powers / jnp.sum(powers, axis=-1, keepdims=True)).astype(BF16)
        out = jnp.dot(probs, values, preferred_element_type=F32)
        mixed[rows, head * HD : (head + 1) * HD] = out.astype(BF16)


def own_qkv_kernel(parts, *refs):
    chunks, (gain, bias, weights, qkv, hidden) = refs[:parts], refs[parts:]
    at = 0
    for chunk in chunks:
        rows = chunk.shape[0]
        hidden[at : at + rows] = normed(chunk[...], gain[...], bias[...])
        at += rows
    project(hidden[...], weights, qkv)


def others_kernel(parts, pieces, spare, *refs):
    chunks, alone, refs = refs[:parts], refs[parts : parts + spare], refs[:parts] + refs[parts + spare :]
    first = lax.axis_index("section") == 0
    gain, bias, w_in, w_out, mine = refs[parts : parts + 5]
    qkv = refs[parts + 5]
    outs = refs[parts + 6 : parts + 6 + pieces]
    hidden, mixed = refs[parts + 6 + pieces :]
    at = 0
    for chunk in chunks:
        rows = chunk.shape[0]
        value = chunk[...]
        if alone:
            start = at % alone[0].shape[0]
            value = jnp.where(first, alone[at // alone[0].shape[0]][start : start + rows], value)
        hidden[at : at + rows] = normed(value, gain[...], bias[...])
        at += rows
    project(hidden[...], w_in, qkv)
    attend(qkv, (mine, qkv), slice(0, at), mixed)
    project(mixed[...], w_out, *outs)


def own_kernel(mine, theirs, w_out, out, mixed):
    attend(mine, (mine, theirs), slice(0, mine.shape[0]), mixed)
    project(mixed[...], w_out, out)


def combine_kernel(start, *refs):
    current, own, got, result = refs[0], refs[1], refs[2:-1], refs[-1]
    rows = slice(start, start + result.shape[0])
    total = own[rows].astype(F32)
    for piece in got:
        total = total + piece[...].astype(F32)
    result[...] = (current[...].astype(F32) + total).astype(BF16)


def next_kernel(start, order, arriving, other, following):
    first = lax.axis_index("section") == 0
    take = jnp.logical_and(order[0, 0] == order[0, 1], jnp.logical_not(first))
    rows = slice(start, start + following.shape[0])
    following[...] = jnp.where(take, arriving[...], other[rows])


def held_kernel(parts, order, acts, fresh, *refs):
    arrived, held = refs[:parts], refs[parts]
    first = lax.axis_index("section") == 0
    for slot in range(acts.shape[1]):
        old, new = order[0, 0] == slot, order[0, 1] == slot
        at = 0
        for chunk in arrived:
            rows = slice(at, at + chunk.shape[0])
            value = jnp.where(first, fresh[0, rows], chunk[...])
            value = jnp.where(old, value, acts[0, slot, rows])
            held[0, slot, rows] = jnp.where(new, fresh[1, rows], value)
            at += chunk.shape[0]


def put_kernel(tick, parts, *refs):
    chunks, out, sems = refs[:parts], refs[-2], refs[-1]
    copies = []
    at = 0
    for i, chunk in enumerate(chunks):
        rows = pl.ds(at, chunk.shape[0])
        copies.append(pltpu.make_async_copy(chunk, out.at[tick, 0, rows], sems.at[i]))
        at += chunk.shape[0]
    for copy in copies:
        copy.start()
    for copy in copies:
        copy.wait()


def last_kernel(pieces, order, *refs):
    chunks, out, sems = refs[: len(pieces)], refs[-2], refs[-1]

    @pl.when(lax.axis_index("section") > 0)
    def _():
        copies = []
        for i, (chunk, (start, size)) in enumerate(zip(chunks, pieces)):
            target = out.at[0, order[0, 1], pl.ds(start, size)]
            copies.append(pltpu.make_async_copy(chunk, target, sems.at[i]))
        for copy in copies:
            copy.start()
        for copy in copies:
            copy.wait()


def cuts(rows, shares):
    sizes = [max(16, rows * share // sum(shares)) for share in shares]
    return [(sum(sizes[:i]), size) for i, size in enumerate(sizes)]


def layer(pieces, chunks, got, gain, bias, w_in, w_out, alone=()):
    size = lax.axis_size("tensor")
    sections = range(lax.axis_size("section"))
    parts = len(chunks)
    rows = sum(c.shape[0] for c in chunks)
    wide, deep = w_in.shape[1], w_out.shape[0]
    width = w_in.shape[0]
    mine = call(
        functools.partial(own_qkv_kernel, parts),
        inner((rows, wide)),
        VMEM,
        [VMEM] * (parts + 3),
        [*chunks, gain, bias, w_in],
        flops=2 * rows * width * wide,
        scratch=[inner((rows, width))],
    )
    far = (size - 1) * rows
    count = (size - 1) * len(pieces)
    theirs, *sends = call(
        functools.partial(others_kernel, len(got), count, len(alone)),
        [inner((far, wide))] + [inner((n, width)) for _ in range(size - 1) for _, n in pieces],
        [VMEM] * (count + 1),
        [VMEM] * (len(got) + len(alone) + 5),
        [*got, *alone, gain, bias, w_in, w_out, mine],
        flops=2 * far * width * wide,
        scratch=[inner((far, width)), inner((far, deep))],
    )
    returned = []
    for i in range(len(pieces)):
        parts_of_i = [rotate(sends[(j - 1) * len(pieces) + i], -j, sections) for j in range(1, size)]
        returned.append(parts_of_i)
    own = call(
        own_kernel,
        inner((rows, width)),
        VMEM,
        [VMEM] * 3,
        [mine, theirs, w_out],
        flops=2 * rows * width * deep,
        scratch=[inner((rows, deep))],
    )
    return own, returned


def body(acts, fresh, order, ln_gain, ln_bias, wqkv, wo):
    rows, width = acts.shape[2:]
    ticks = fresh.shape[0]
    dma = pltpu.SemaphoreType.DMA
    acts, fresh, order, wqkv, wo = map(outside, (acts, fresh, order, wqkv, wo))
    current, order = call(
        pick_kernel,
        [inner((rows, width)), pltpu.SMEM(order.shape, order.dtype)],
        [VMEM, SMEM],
        [ANY, ANY],
        [order, acts],
        scratch=[inner(acts.shape[1:]), dma((2,))],
    )
    other = call(other_kernel, inner((rows, width)), VMEM, [SMEM, ANY, ANY], [order, acts, fresh], scratch=[dma((2,))])
    w_in, w_out = call(
        weights_kernel,
        [inner(wqkv.shape[1:]), inner(wo.shape[1:])],
        [VMEM, VMEM],
        [ANY, ANY],
        [wqkv, wo],
        scratch=[dma((5,))],
        limit=24,
        flops=1 << 30,
    )
    shifts = range(1, lax.axis_size("tensor"))
    sections = range(lax.axis_size("section"))
    chunks = [current]
    got = [rotate(current, j, sections) for j in shifts]
    alone = [rotate(other, j, [0]) for j in shifts]
    section_out = held = None
    for tick in range(ticks):
        here_at = [sum(c.shape[0] for c in chunks[:i]) for i in range(len(chunks))]
        if tick:
            before, parts = arrived, len(arrived)
        pieces = cuts(rows, SHARES[tick])
        own, returned = layer(pieces, chunks, got, ln_gain, ln_bias, w_in, w_out, alone if tick else ())
        ready = []
        if tick:
            section_out = call(
                functools.partial(put_kernel, 0, parts),
                pltpu.HBM((ticks, 1, rows, width), BF16),
                ANY,
                [VMEM] * parts,
                results,
                scratch=[dma((parts,))],
                wait=[own],
            )
            held = call(
                functools.partial(held_kernel, parts),
                pltpu.HBM(acts.shape, BF16),
                VMEM,
                [SMEM, VMEM, VMEM] + [VMEM] * parts,
                [order, acts, fresh, *before],
                wait=[own],
            )
            section_out, held = outside(section_out), outside(held)
            ready = [section_out, held]
        results, arrived = [], []
        for i, (start, size) in enumerate(pieces):

            holder = max(k for k, at in enumerate(here_at) if at <= start)

            def combine(*refs, start=start, size=size, at=here_at[holder]):
                combine_kernel(start, refs[0].at[pl.ds(start - at, size)], *refs[1:])

            result = call(
                combine,
                inner((size, width)),
                VMEM,
                [VMEM] * (2 + len(returned[i])),
                [chunks[holder], own, *returned[i]],
                wait=ready,
            )
            results.append(result)
            arrived.append(held_inside(from_behind(result, "section")))
        if tick == 0:
            chunks, swapped = [], []
            for i, (start, size) in enumerate(pieces):
                chunks.append(
                    call(
                        functools.partial(next_kernel, start),
                        inner((size, width)),
                        VMEM,
                        [SMEM, VMEM, VMEM],
                        [order, arrived[i], other],
                    )
                )
                swapped.append([rotate(chunks[i], j, sections[1:], rest=True) for j in shifts])
            got = [block for of_j in zip(*swapped) for block in of_j]
    parts = len(pieces)
    section_out = call(
        functools.partial(put_kernel, ticks - 1, parts),
        pltpu.HBM((ticks, 1, rows, width), BF16),
        ANY,
        [VMEM] * parts + [ANY],
        [*results, section_out],
        scratch=[dma((parts,))],
        aliases={parts: 0},
    )
    for which in (range(parts - 1), range(parts - 1, parts)):
        held = call(
            functools.partial(last_kernel, [pieces[i] for i in which]),
            pltpu.HBM(acts.shape, BF16),
            ANY,
            [SMEM] + [VMEM] * len(which) + [ANY],
            [order, *(arrived[i] for i in which), outside(held)],
            scratch=[dma((len(which),))],
            aliases={len(which) + 1: 0},
        )
    return section_out, held


def solution(mesh):
    return jax.shard_map(
        body,
        mesh=mesh,
        in_specs=(
            P("section", "dp", "tensor", None),
            P("dp", "tensor", None),
            P("section", None),
            P("section", None),
            P("section", None),
            P("section", None, "tensor"),
            P("section", "tensor", None),
        ),
        out_specs=(P("dp", "section", "tensor", None), P("section", "dp", "tensor", None)),
        check_vma=False,
    )
```

```python
import functools

import jax
import jax.numpy as jnp
from jax import lax
from jax.experimental import pallas as pl
from jax.experimental.pallas import tpu as pltpu
from jax.sharding import PartitionSpec as P


HD = 128
SHARES = ((1, 1), (2, 1, 1))
MIB = 1 << 20
F32 = jnp.float32
BF16 = jnp.bfloat16

VMEM = pl.BlockSpec(memory_space=pltpu.VMEM)
SMEM = pl.BlockSpec(memory_space=pltpu.SMEM)
ANY = pl.BlockSpec(memory_space=pl.ANY)


def inner(shape, dtype=BF16):
    return pltpu.VMEM(tuple(shape), dtype)


def held_inside(block):
    return pltpu.with_memory_space_constraint(block, pltpu.VMEM)


def outside(block):
    return pltpu.with_memory_space_constraint(block, pltpu.HBM)


def after(kernel, count):
    return lambda *refs: kernel(*refs[count:])


def call(kernel, outs, out_specs, in_specs, args, flops=0, scratch=(), aliases=None, limit=16, wait=()):
    if wait:
        kernel = after(kernel, len(wait))
        in_specs, args = [ANY] * len(wait) + in_specs, [*wait, *args]
        aliases = {k + len(wait): v for k, v in (aliases or {}).items()}
    return pl.pallas_call(
        kernel,
        out_shape=outs,
        out_specs=out_specs,
        in_specs=in_specs,
        scratch_shapes=list(scratch),
        input_output_aliases=aliases or {},
        compiler_params=pltpu.CompilerParams(vmem_limit_bytes=limit * MIB),
        cost_estimate=pl.CostEstimate(flops=max(flops, 1 << 20), bytes_accessed=1 << 16, transcendentals=0),
    )(*args)


RING = (False, True)


def from_behind(block, axis, ring):
    size = lax.axis_size(axis)
    return lax.ppermute(block, axis, [(i, (i + 1) % size) for i in range(size - 1 + ring)])


def rotate(block, shift, sections, rest=False):
    names = ("section", "tensor", "dp")
    count, size, groups = map(lax.axis_size, names)
    route = []
    for s in range(count):
        for i in range(size):
            for d in range(groups):
                here = (s * size + i) * groups + d
                if s in sections:
                    route.append((here, (s * size + (i + shift) % size) * groups + d))
                elif rest and d ^ 1 < groups:
                    route.append((here, here - d + (d ^ 1)))
    return held_inside(lax.ppermute(block, names, route))


def pick_kernel(order, acts, current, kept, slots, sems):
    number = pltpu.make_async_copy(order, kept, sems.at[0])
    blocks = pltpu.make_async_copy(acts.at[0], slots, sems.at[1])
    number.start()
    blocks.start()
    number.wait()
    blocks.wait()
    current[...] = slots[kept[0, 0]]


def weights_kernel(w_in, w_out, in_inside, out_inside, sems):
    copies = []
    pieces = 4
    step = w_in.shape[1] // pieces
    for i in range(pieces):
        rows = pl.ds(i * step, step)
        copies.append(pltpu.make_async_copy(w_in.at[0, rows], in_inside.at[rows], sems.at[i]))
    copies.append(pltpu.make_async_copy(w_out.at[0], out_inside, sems.at[pieces]))
    for copy in copies:
        copy.start()
    for copy in copies:
        copy.wait()


def other_kernel(order, acts, fresh, other, sems):
    first = lax.axis_index("section") == 0
    repeated = order[0, 0] == order[0, 1]
    copy = pltpu.make_async_copy(acts.at[0, order[0, 1]], other, sems.at[0])
    copy.start()
    copy.wait()

    @pl.when(jnp.logical_and(first, repeated))
    def _():
        again = pltpu.make_async_copy(fresh.at[0], other, sems.at[1])
        again.start()
        again.wait()


def normed(rows, gain, bias):
    values = rows.astype(F32)
    centred = values - jnp.mean(values, axis=-1, keepdims=True)
    spread = jnp.mean(centred * centred, axis=-1, keepdims=True)
    return (centred * lax.rsqrt(spread + 1e-06) * gain + bias).astype(BF16)


def project(rows, weights, *targets, width=1024):
    for start in range(0, weights.shape[1], width):
        columns = slice(start, min(start + width, weights.shape[1]))
        value = jnp.dot(rows, weights[:, columns], preferred_element_type=F32).astype(BF16)
        at = 0
        for target in targets:
            target[:, columns] = value[at : at + target.shape[0]]
            at += target.shape[0]


def attend(q, blocks, rows, mixed):
    heads = q.shape[1] // (3 * HD)
    ones = jnp.ones((sum(b.shape[0] for b in blocks), HD), BF16)
    for head in range(heads):
        at = [slice((head * 3 + j) * HD, (head * 3 + j + 1) * HD) for j in range(3)]
        query = q[rows, at[0]]
        keys = jnp.concatenate([b[:, at[1]] for b in blocks], axis=0)
        values = jnp.concatenate([b[:, at[2]] for b in blocks], axis=0)
        scores = lax.dot_general(query, keys, (((1,), (1,)), ((), ())), preferred_element_type=F32)
        powers = jnp.exp((scores - jnp.max(scores, axis=-1, keepdims=True)) * (1.0 / HD**0.5)).astype(BF16)
        out = jnp.dot(powers, jnp.concatenate([values, ones], axis=1), preferred_element_type=F32)
        mixed[rows, head * HD : (head + 1) * HD] = (out[:, :HD] / out[:, HD:]).astype(BF16)


def own_qkv_kernel(parts, *refs):
    chunks, (gain, bias, weights, qkv, hidden) = refs[:parts], refs[parts:]
    at = 0
    for chunk in chunks:
        rows = chunk.shape[0]
        hidden[at : at + rows] = normed(chunk[...], gain[...], bias[...])
        at += rows
    project(hidden[...], weights, qkv)


def others_kernel(parts, pieces, spare, *refs):
    chunks, alone, refs = refs[:parts], refs[parts : parts + spare], refs[:parts] + refs[parts + spare :]
    first = lax.axis_index("section") == 0
    gain, bias, w_in, w_out, mine = refs[parts : parts + 5]
    qkv = refs[parts + 5]
    outs = refs[parts + 6 : parts + 6 + pieces]
    hidden, mixed = refs[parts + 6 + pieces :]
    at = 0
    for chunk in chunks:
        rows = chunk.shape[0]
        value = chunk[...]
        if alone:
            start = at % alone[0].shape[0]
            value = jnp.where(first, alone[at // alone[0].shape[0]][start : start + rows], value)
        hidden[at : at + rows] = normed(value, gain[...], bias[...])
        at += rows
    project(hidden[...], w_in, qkv)
    attend(qkv, (mine, qkv), slice(0, at), mixed)
    project(mixed[...], w_out, *outs)


def own_kernel(mine, theirs, w_out, out, mixed):
    attend(mine, (mine, theirs), slice(0, mine.shape[0]), mixed)
    project(mixed[...], w_out, out)


def combine_kernel(start, *refs):
    current, own, got, result = refs[0], refs[1], refs[2:-1], refs[-1]
    rows = slice(start, start + result.shape[0])
    total = own[rows].astype(F32)
    for piece in got:
        total = total + piece[...].astype(F32)
    result[...] = (current[...].astype(F32) + total).astype(BF16)


def next_kernel(start, order, arriving, other, following):
    first = lax.axis_index("section") == 0
    take = jnp.logical_and(order[0, 0] == order[0, 1], jnp.logical_not(first))
    rows = slice(start, start + following.shape[0])
    following[...] = jnp.where(take, arriving[...], other[rows])


def held_kernel(parts, order, acts, fresh, *refs):
    arrived, held = refs[:parts], refs[parts]
    first = lax.axis_index("section") == 0
    for slot in range(acts.shape[1]):
        old, new = order[0, 0] == slot, order[0, 1] == slot
        at = 0
        for chunk in arrived:
            rows = slice(at, at + chunk.shape[0])
            value = jnp.where(first, fresh[0, rows], chunk[...])
            value = jnp.where(old, value, acts[0, slot, rows])
            held[0, slot, rows] = jnp.where(new, fresh[1, rows], value)
            at += chunk.shape[0]


def put_kernel(tick, parts, *refs):
    chunks, out, sems = refs[:parts], refs[-2], refs[-1]
    copies = []
    at = 0
    for i, chunk in enumerate(chunks):
        rows = pl.ds(at, chunk.shape[0])
        copies.append(pltpu.make_async_copy(chunk, out.at[tick, 0, rows], sems.at[i]))
        at += chunk.shape[0]
    for copy in copies:
        copy.start()
    for copy in copies:
        copy.wait()


def last_kernel(pieces, order, *refs):
    chunks, out, sems = refs[: len(pieces)], refs[-2], refs[-1]

    @pl.when(lax.axis_index("section") > 0)
    def _():
        copies = []
        for i, (chunk, (start, size)) in enumerate(zip(chunks, pieces)):
            target = out.at[0, order[0, 1], pl.ds(start, size)]
            copies.append(pltpu.make_async_copy(chunk, target, sems.at[i]))
        for copy in copies:
            copy.start()
        for copy in copies:
            copy.wait()


def cuts(rows, shares):
    units = rows // 16
    edges = [units * sum(shares[:i]) // sum(shares) * 16 for i in range(len(shares))] + [rows]
    return [(a, b - a) for a, b in zip(edges, edges[1:]) if b > a]


def layer(pieces, chunks, got, gain, bias, w_in, w_out, alone=()):
    size = lax.axis_size("tensor")
    sections = range(lax.axis_size("section"))
    parts = len(chunks)
    rows = sum(c.shape[0] for c in chunks)
    wide, deep = w_in.shape[1], w_out.shape[0]
    width = w_in.shape[0]
    mine = call(
        functools.partial(own_qkv_kernel, parts),
        inner((rows, wide)),
        VMEM,
        [VMEM] * (parts + 3),
        [*chunks, gain, bias, w_in],
        flops=2 * rows * width * wide,
        scratch=[inner((rows, width))],
    )
    far = (size - 1) * rows
    count = (size - 1) * len(pieces)
    theirs, *sends = call(
        functools.partial(others_kernel, len(got), count, len(alone)),
        [inner((far, wide))] + [inner((n, width)) for _ in range(size - 1) for _, n in pieces],
        [VMEM] * (count + 1),
        [VMEM] * (len(got) + len(alone) + 5),
        [*got, *alone, gain, bias, w_in, w_out, mine],
        flops=2 * far * width * wide,
        scratch=[inner((far, width)), inner((far, deep))],
    )
    returned = []
    for i in range(len(pieces)):
        parts_of_i = [rotate(sends[(j - 1) * len(pieces) + i], -j, sections) for j in range(1, size)]
        returned.append(parts_of_i)
    own = call(
        own_kernel,
        inner((rows, width)),
        VMEM,
        [VMEM] * 3,
        [mine, theirs, w_out],
        flops=2 * rows * width * deep,
        scratch=[inner((rows, deep))],
    )
    return own, returned


def body(acts, fresh, order, ln_gain, ln_bias, wqkv, wo):
    rows, width = acts.shape[2:]
    ticks = fresh.shape[0]
    dma = pltpu.SemaphoreType.DMA
    acts, fresh, order, wqkv, wo = map(outside, (acts, fresh, order, wqkv, wo))
    current, order = call(
        pick_kernel,
        [inner((rows, width)), pltpu.SMEM(order.shape, order.dtype)],
        [VMEM, SMEM],
        [ANY, ANY],
        [order, acts],
        scratch=[inner(acts.shape[1:]), dma((2,))],
    )
    other = call(other_kernel, inner((rows, width)), VMEM, [SMEM, ANY, ANY], [order, acts, fresh], scratch=[dma((2,))])
    w_in, w_out = call(
        weights_kernel,
        [inner(wqkv.shape[1:]), inner(wo.shape[1:])],
        [VMEM, VMEM],
        [ANY, ANY],
        [wqkv, wo],
        scratch=[dma((5,))],
        limit=24,
        flops=1 << 30,
    )
    shifts = range(1, lax.axis_size("tensor"))
    sections = range(lax.axis_size("section"))
    chunks = [current]
    got = [rotate(current, j, sections) for j in shifts]
    alone = [rotate(other, j, [0]) for j in shifts]
    section_out = held = None
    for tick in range(ticks):
        here_at = [sum(c.shape[0] for c in chunks[:i]) for i in range(len(chunks))]
        if tick:
            before, parts = arrived, len(arrived)
        pieces = cuts(rows, SHARES[tick])
        own, returned = layer(pieces, chunks, got, ln_gain, ln_bias, w_in, w_out, alone if tick else ())
        ready = []
        if tick:
            section_out = call(
                functools.partial(put_kernel, 0, parts),
                pltpu.HBM((ticks, 1, rows, width), BF16),
                ANY,
                [VMEM] * parts,
                results,
                scratch=[dma((parts,))],
                wait=[own],
            )
            held = call(
                functools.partial(held_kernel, parts),
                pltpu.HBM(acts.shape, BF16),
                VMEM,
                [SMEM, VMEM, VMEM] + [VMEM] * parts,
                [order, acts, fresh, *before],
                wait=[own],
            )
            section_out, held = outside(section_out), outside(held)
            ready = [section_out, held]
        results, arrived = [], []
        for i, (start, size) in enumerate(pieces):

            holder = max(k for k, at in enumerate(here_at) if at <= start)

            def combine(*refs, start=start, size=size, at=here_at[holder]):
                combine_kernel(start, refs[0].at[pl.ds(start - at, size)], *refs[1:])

            result = call(
                combine,
                inner((size, width)),
                VMEM,
                [VMEM] * (2 + len(returned[i])),
                [chunks[holder], own, *returned[i]],
                wait=ready,
            )
            results.append(result)
            arrived.append(held_inside(from_behind(result, "section", RING[tick])))
        if tick == 0:
            chunks, swapped = [], []
            for i, (start, size) in enumerate(pieces):
                chunks.append(
                    call(
                        functools.partial(next_kernel, start),
                        inner((size, width)),
                        VMEM,
                        [SMEM, VMEM, VMEM],
                        [order, arrived[i], other],
                    )
                )
                swapped.append([rotate(chunks[i], j, sections[1:], rest=True) for j in shifts])
            got = [block for of_j in zip(*swapped) for block in of_j]
    parts = len(pieces)
    section_out = call(
        functools.partial(put_kernel, ticks - 1, parts),
        pltpu.HBM((ticks, 1, rows, width), BF16),
        ANY,
        [VMEM] * parts + [ANY],
        [*results, section_out],
        scratch=[dma((parts,))],
        aliases={parts: 0},
    )
    for which in (range(parts - 1), range(parts - 1, parts)):
        held = call(
            functools.partial(last_kernel, [pieces[i] for i in which]),
            pltpu.HBM(acts.shape, BF16),
            ANY,
            [SMEM] + [VMEM] * len(which) + [ANY],
            [order, *(arrived[i] for i in which), outside(held)],
            scratch=[dma((len(which),))],
            aliases={len(which) + 1: 0},
        )
    return section_out, held


def solution(mesh):
    return jax.shard_map(
        body,
        mesh=mesh,
        in_specs=(
            P("section", "dp", "tensor", None),
            P("dp", "tensor", None),
            P("section", None),
            P("section", None),
            P("section", None),
            P("section", None, "tensor"),
            P("section", "tensor", None),
        ),
        out_specs=(P("dp", "section", "tensor", None), P("section", "dp", "tensor", None)),
        check_vma=False,
    )
```

```python
import functools

import jax
import jax.numpy as jnp
from jax import lax
from jax.experimental import pallas as pl
from jax.experimental.pallas import tpu as pltpu
from jax.sharding import PartitionSpec as P


HD = 128
SHARES = ((1, 1), (2, 1, 1))
MIB = 1 << 20
F32 = jnp.float32
BF16 = jnp.bfloat16

VMEM = pl.BlockSpec(memory_space=pltpu.VMEM)
SMEM = pl.BlockSpec(memory_space=pltpu.SMEM)
ANY = pl.BlockSpec(memory_space=pl.ANY)


def inner(shape, dtype=BF16):
    return pltpu.VMEM(tuple(shape), dtype)


def held_inside(block):
    return pltpu.with_memory_space_constraint(block, pltpu.VMEM)


def outside(block):
    return pltpu.with_memory_space_constraint(block, pltpu.HBM)


def after(kernel, count):
    return lambda *refs: kernel(*refs[count:])


def call(kernel, outs, out_specs, in_specs, args, flops=0, scratch=(), aliases=None, limit=16, wait=()):
    if wait:
        kernel = after(kernel, len(wait))
        in_specs, args = [ANY] * len(wait) + in_specs, [*wait, *args]
        aliases = {k + len(wait): v for k, v in (aliases or {}).items()}
    return pl.pallas_call(
        kernel,
        out_shape=outs,
        out_specs=out_specs,
        in_specs=in_specs,
        scratch_shapes=list(scratch),
        input_output_aliases=aliases or {},
        compiler_params=pltpu.CompilerParams(vmem_limit_bytes=limit * MIB),
        cost_estimate=pl.CostEstimate(flops=max(flops, 1 << 20), bytes_accessed=1 << 16, transcendentals=0),
    )(*args)


RING = (False, True)


def from_behind(block, axis, ring):
    size = lax.axis_size(axis)
    return lax.ppermute(block, axis, [(i, (i + 1) % size) for i in range(size - 1 + ring)])


def rotate(block, shift, sections, rest=False):
    names = ("section", "tensor", "dp")
    count, size, groups = map(lax.axis_size, names)
    route = []
    for s in range(count):
        for i in range(size):
            for d in range(groups):
                here = (s * size + i) * groups + d
                if s in sections:
                    route.append((here, (s * size + (i + shift) % size) * groups + d))
                elif rest and d ^ 1 < groups:
                    route.append((here, here - d + (d ^ 1)))
    return held_inside(lax.ppermute(block, names, route))


def pick_kernel(parts, order, acts, *refs):
    chunks, (kept, slots, sems) = refs[:parts], refs[parts:]
    number = pltpu.make_async_copy(order, kept, sems.at[0])
    blocks = pltpu.make_async_copy(acts.at[0], slots, sems.at[1])
    number.start()
    blocks.start()
    number.wait()
    blocks.wait()
    at = 0
    for chunk in chunks:
        chunk[...] = slots[kept[0, 0], at : at + chunk.shape[0]]
        at += chunk.shape[0]


def weights_kernel(w_in, w_out, in_inside, out_inside, sems):
    copies = []
    pieces = 4
    step = w_in.shape[1] // pieces
    for i in range(pieces):
        rows = pl.ds(i * step, step)
        copies.append(pltpu.make_async_copy(w_in.at[0, rows], in_inside.at[rows], sems.at[i]))
    copies.append(pltpu.make_async_copy(w_out.at[0], out_inside, sems.at[pieces]))
    for copy in copies:
        copy.start()
    for copy in copies:
        copy.wait()


def other_kernel(order, acts, fresh, other, sems):
    first = lax.axis_index("section") == 0
    repeated = order[0, 0] == order[0, 1]
    copy = pltpu.make_async_copy(acts.at[0, order[0, 1]], other, sems.at[0])
    copy.start()
    copy.wait()

    @pl.when(jnp.logical_and(first, repeated))
    def _():
        again = pltpu.make_async_copy(fresh.at[0], other, sems.at[1])
        again.start()
        again.wait()


def normed(rows, gain, bias):
    values = rows.astype(F32)
    centred = values - jnp.mean(values, axis=-1, keepdims=True)
    spread = jnp.mean(centred * centred, axis=-1, keepdims=True)
    return (centred * lax.rsqrt(spread + 1e-06) * gain + bias).astype(BF16)


def project(rows, weights, *targets, width=1024):
    for start in range(0, weights.shape[1], width):
        columns = slice(start, min(start + width, weights.shape[1]))
        value = jnp.dot(rows, weights[:, columns], preferred_element_type=F32).astype(BF16)
        at = 0
        for target in targets:
            target[:, columns] = value[at : at + target.shape[0]]
            at += target.shape[0]


def attend(q, blocks, rows, mixed):
    heads = q.shape[1] // (3 * HD)
    ones = jnp.ones((sum(b.shape[0] for b in blocks), HD), BF16)
    for head in range(heads):
        at = [slice((head * 3 + j) * HD, (head * 3 + j + 1) * HD) for j in range(3)]
        query = q[rows, at[0]]
        keys = jnp.concatenate([b[:, at[1]] for b in blocks], axis=0)
        values = jnp.concatenate([b[:, at[2]] for b in blocks], axis=0)
        scores = lax.dot_general(query, keys, (((1,), (1,)), ((), ())), preferred_element_type=F32)
        powers = jnp.exp((scores - jnp.max(scores, axis=-1, keepdims=True)) * (1.0 / HD**0.5)).astype(BF16)
        out = jnp.dot(powers, jnp.concatenate([values, ones], axis=1), preferred_element_type=F32)
        mixed[rows, head * HD : (head + 1) * HD] = (out[:, :HD] / out[:, HD:]).astype(BF16)


def own_qkv_kernel(parts, *refs):
    chunks, (gain, bias, weights, qkv, hidden) = refs[:parts], refs[parts:]
    at = 0
    for chunk in chunks:
        rows = chunk.shape[0]
        hidden[at : at + rows] = normed(chunk[...], gain[...], bias[...])
        at += rows
    project(hidden[...], weights, qkv)


def chosen(chunk, alone, j, start):
    value = chunk[...]
    if alone:
        mine = alone[j][start : start + chunk.shape[0]]
        value = jnp.where(lax.axis_index("section") == 0, mine, value)
    return value


def ahead_kernel(blocks, spare, *refs):
    firsts, alone, (gain, bias, hidden) = refs[:blocks], refs[blocks : blocks + spare], refs[blocks + spare :]
    for j, chunk in enumerate(firsts):
        rows = chunk.shape[0]
        hidden[j * rows : (j + 1) * rows] = normed(chosen(chunk, alone, j, 0), gain[...], bias[...])


def others_kernel(blocks, parts, spare, *refs):
    count = blocks * (parts - 1)
    ready, chunks, alone = refs[0], refs[1 : 1 + count], refs[1 + count : 1 + count + spare]
    gain, bias, w_in, w_out, mine, qkv, *outs, hidden, mixed = refs[1 + count + spare :]
    rows, first = hidden.shape[0] // blocks, ready.shape[0] // blocks
    for j in range(blocks):
        hidden[j * rows : j * rows + first] = ready[j * first : (j + 1) * first]
        at = first
        for chunk in chunks[j * (parts - 1) : (j + 1) * (parts - 1)]:
            here = slice(j * rows + at, j * rows + at + chunk.shape[0])
            hidden[here] = normed(chosen(chunk, alone, j, at), gain[...], bias[...])
            at += chunk.shape[0]
    project(hidden[...], w_in, qkv)
    attend(qkv, (mine, qkv), slice(0, hidden.shape[0]), mixed)
    project(mixed[...], w_out, *outs)


def own_kernel(mine, theirs, w_out, out, mixed):
    attend(mine, (mine, theirs), slice(0, mine.shape[0]), mixed)
    project(mixed[...], w_out, out)


def combine_kernel(start, *refs):
    current, own, got, result = refs[0], refs[1], refs[2:-1], refs[-1]
    rows = slice(start, start + result.shape[0])
    total = own[rows].astype(F32)
    for piece in got:
        total = total + piece[...].astype(F32)
    result[...] = (current[...].astype(F32) + total).astype(BF16)


def next_kernel(start, order, arriving, other, following):
    first = lax.axis_index("section") == 0
    take = jnp.logical_and(order[0, 0] == order[0, 1], jnp.logical_not(first))
    rows = slice(start, start + following.shape[0])
    following[...] = jnp.where(take, arriving[...], other[rows])


def held_kernel(parts, order, acts, fresh, *refs):
    arrived, held = refs[:parts], refs[parts]
    first = lax.axis_index("section") == 0
    for slot in range(acts.shape[1]):
        old, new = order[0, 0] == slot, order[0, 1] == slot
        at = 0
        for chunk in arrived:
            rows = slice(at, at + chunk.shape[0])
            value = jnp.where(first, fresh[0, rows], chunk[...])
            value = jnp.where(old, value, acts[0, slot, rows])
            held[0, slot, rows] = jnp.where(new, fresh[1, rows], value)
            at += chunk.shape[0]


def put_kernel(tick, parts, *refs):
    chunks, out, sems = refs[:parts], refs[-2], refs[-1]
    copies = []
    at = 0
    for i, chunk in enumerate(chunks):
        rows = pl.ds(at, chunk.shape[0])
        copies.append(pltpu.make_async_copy(chunk, out.at[tick, 0, rows], sems.at[i]))
        at += chunk.shape[0]
    for copy in copies:
        copy.start()
    for copy in copies:
        copy.wait()


def last_kernel(pieces, order, *refs):
    chunks, out, sems = refs[: len(pieces)], refs[-2], refs[-1]

    @pl.when(lax.axis_index("section") > 0)
    def _():
        copies = []
        for i, (chunk, (start, size)) in enumerate(zip(chunks, pieces)):
            target = out.at[0, order[0, 1], pl.ds(start, size)]
            copies.append(pltpu.make_async_copy(chunk, target, sems.at[i]))
        for copy in copies:
            copy.start()
        for copy in copies:
            copy.wait()


def cuts(rows, shares):
    units = rows // 16
    edges = [units * sum(shares[:i]) // sum(shares) * 16 for i in range(len(shares))] + [rows]
    return [(a, b - a) for a, b in zip(edges, edges[1:]) if b > a]


def layer(pieces, chunks, got, gain, bias, w_in, w_out, alone=()):
    size = lax.axis_size("tensor")
    sections = range(lax.axis_size("section"))
    parts = len(chunks)
    rows = sum(c.shape[0] for c in chunks)
    wide, deep = w_in.shape[1], w_out.shape[0]
    width = w_in.shape[0]
    mine = call(
        functools.partial(own_qkv_kernel, parts),
        inner((rows, wide)),
        VMEM,
        [VMEM] * (parts + 3),
        [*chunks, gain, bias, w_in],
        flops=2 * rows * width * wide,
        scratch=[inner((rows, width))],
    )
    far = (size - 1) * rows
    count = (size - 1) * len(pieces)
    blocks = size - 1
    each = len(got) // blocks
    firsts = got[::each]
    rest = [block for i, block in enumerate(got) if i % each]
    ready = call(
        functools.partial(ahead_kernel, blocks, len(alone)),
        inner((sum(block.shape[0] for block in firsts), width)),
        VMEM,
        [VMEM] * (blocks + len(alone) + 2),
        [*firsts, *alone, gain, bias],
        wait=[mine],
    )
    theirs, *sends = call(
        functools.partial(others_kernel, blocks, each, len(alone)),
        [inner((far, wide))] + [inner((n, width)) for _ in range(size - 1) for _, n in pieces],
        [VMEM] * (count + 1),
        [VMEM] * (len(rest) + len(alone) + 6),
        [ready, *rest, *alone, gain, bias, w_in, w_out, mine],
        flops=2 * far * width * wide,
        scratch=[inner((far, width)), inner((far, deep))],
    )
    returned = []
    for i in range(len(pieces)):
        parts_of_i = [rotate(sends[(j - 1) * len(pieces) + i], -j, sections) for j in range(1, size)]
        returned.append(parts_of_i)
    own = call(
        own_kernel,
        inner((rows, width)),
        VMEM,
        [VMEM] * 3,
        [mine, theirs, w_out],
        flops=2 * rows * width * deep,
        scratch=[inner((rows, deep))],
    )
    return own, returned


def body(acts, fresh, order, ln_gain, ln_bias, wqkv, wo):
    rows, width = acts.shape[2:]
    ticks = fresh.shape[0]
    dma = pltpu.SemaphoreType.DMA
    acts, fresh, order, wqkv, wo = map(outside, (acts, fresh, order, wqkv, wo))
    pieces = cuts(rows, (1,))
    *chunks, order = call(
        functools.partial(pick_kernel, len(pieces)),
        [*(inner((size, width)) for _, size in pieces), pltpu.SMEM(order.shape, order.dtype)],
        [VMEM] * len(pieces) + [SMEM],
        [ANY, ANY],
        [order, acts],
        scratch=[inner(acts.shape[1:]), dma((2,))],
    )
    other = call(other_kernel, inner((rows, width)), VMEM, [SMEM, ANY, ANY], [order, acts, fresh], scratch=[dma((2,))])
    w_in, w_out = call(
        weights_kernel,
        [inner(wqkv.shape[1:]), inner(wo.shape[1:])],
        [VMEM, VMEM],
        [ANY, ANY],
        [wqkv, wo],
        scratch=[dma((5,))],
        limit=24,
        flops=1 << 30,
    )
    shifts = range(1, lax.axis_size("tensor"))
    sections = range(lax.axis_size("section"))
    got = [rotate(chunk, j, sections) for j in shifts for chunk in chunks]
    alone = [rotate(other, j, [0]) for j in shifts]
    section_out = held = None
    for tick in range(ticks):
        here_at = [sum(c.shape[0] for c in chunks[:i]) for i in range(len(chunks))]
        if tick:
            before, parts = arrived, len(arrived)
        pieces = cuts(rows, SHARES[tick])
        own, returned = layer(pieces, chunks, got, ln_gain, ln_bias, w_in, w_out, alone if tick else ())
        ready = []
        if tick:
            section_out = call(
                functools.partial(put_kernel, 0, parts),
                pltpu.HBM((ticks, 1, rows, width), BF16),
                ANY,
                [VMEM] * parts,
                results,
                scratch=[dma((parts,))],
                wait=[own],
            )
            held = call(
                functools.partial(held_kernel, parts),
                pltpu.HBM(acts.shape, BF16),
                VMEM,
                [SMEM, VMEM, VMEM] + [VMEM] * parts,
                [order, acts, fresh, *before],
                wait=[own],
            )
            section_out, held = outside(section_out), outside(held)
            ready = [section_out, held]
        results, arrived = [], []
        for i, (start, size) in enumerate(pieces):

            holder = max(k for k, at in enumerate(here_at) if at <= start)

            def combine(*refs, start=start, size=size, at=here_at[holder]):
                combine_kernel(start, refs[0].at[pl.ds(start - at, size)], *refs[1:])

            result = call(
                combine,
                inner((size, width)),
                VMEM,
                [VMEM] * (2 + len(returned[i])),
                [chunks[holder], own, *returned[i]],
                wait=ready,
            )
            results.append(result)
            arrived.append(held_inside(from_behind(result, "section", RING[tick])))
        if tick == 0:
            chunks, swapped = [], []
            for i, (start, size) in enumerate(pieces):
                chunks.append(
                    call(
                        functools.partial(next_kernel, start),
                        inner((size, width)),
                        VMEM,
                        [SMEM, VMEM, VMEM],
                        [order, arrived[i], other],
                    )
                )
                swapped.append([rotate(chunks[i], j, sections[1:], rest=True) for j in shifts])
            got = [block for of_j in zip(*swapped) for block in of_j]
    parts = len(pieces)
    section_out = call(
        functools.partial(put_kernel, ticks - 1, parts),
        pltpu.HBM((ticks, 1, rows, width), BF16),
        ANY,
        [VMEM] * parts + [ANY],
        [*results, section_out],
        scratch=[dma((parts,))],
        aliases={parts: 0},
    )
    for which in (range(parts - 1), range(parts - 1, parts)):
        held = call(
            functools.partial(last_kernel, [pieces[i] for i in which]),
            pltpu.HBM(acts.shape, BF16),
            ANY,
            [SMEM] + [VMEM] * len(which) + [ANY],
            [order, *(arrived[i] for i in which), outside(held)],
            scratch=[dma((len(which),))],
            aliases={len(which) + 1: 0},
        )
    return section_out, held


def solution(mesh):
    return jax.shard_map(
        body,
        mesh=mesh,
        in_specs=(
            P("section", "dp", "tensor", None),
            P("dp", "tensor", None),
            P("section", None),
            P("section", None),
            P("section", None),
            P("section", None, "tensor"),
            P("section", "tensor", None),
        ),
        out_specs=(P("dp", "section", "tensor", None), P("section", "dp", "tensor", None)),
        check_vma=False,
    )
```

```python
import functools

import jax
import jax.numpy as jnp
from jax import lax
from jax.experimental import pallas as pl
from jax.experimental.pallas import tpu as pltpu
from jax.sharding import PartitionSpec as P


HD = 128
SHARES = ((1, 1), (2, 1, 1))
MIB = 1 << 20
F32 = jnp.float32
BF16 = jnp.bfloat16

VMEM = pl.BlockSpec(memory_space=pltpu.VMEM)
SMEM = pl.BlockSpec(memory_space=pltpu.SMEM)
ANY = pl.BlockSpec(memory_space=pl.ANY)


def inner(shape, dtype=BF16):
    return pltpu.VMEM(tuple(shape), dtype)


def held_inside(block):
    return pltpu.with_memory_space_constraint(block, pltpu.VMEM)


def outside(block):
    return pltpu.with_memory_space_constraint(block, pltpu.HBM)


def after(kernel, count):
    return lambda *refs: kernel(*refs[count:])


def call(kernel, outs, out_specs, in_specs, args, flops=0, scratch=(), aliases=None, limit=16, wait=()):
    if wait:
        kernel = after(kernel, len(wait))
        in_specs, args = [ANY] * len(wait) + in_specs, [*wait, *args]
        aliases = {k + len(wait): v for k, v in (aliases or {}).items()}
    return pl.pallas_call(
        kernel,
        out_shape=outs,
        out_specs=out_specs,
        in_specs=in_specs,
        scratch_shapes=list(scratch),
        input_output_aliases=aliases or {},
        compiler_params=pltpu.CompilerParams(vmem_limit_bytes=limit * MIB),
        cost_estimate=pl.CostEstimate(flops=max(flops, 1 << 20), bytes_accessed=1 << 16, transcendentals=0),
    )(*args)


RING = (False, True)


def from_behind(block, axis, ring):
    size = lax.axis_size(axis)
    return lax.ppermute(block, axis, [(i, (i + 1) % size) for i in range(size - 1 + ring)])


def rotate(block, shift, sections, rest=False):
    names = ("section", "tensor", "dp")
    count, size, groups = map(lax.axis_size, names)
    route = []
    for s in range(count):
        for i in range(size):
            for d in range(groups):
                here = (s * size + i) * groups + d
                if s in sections:
                    route.append((here, (s * size + (i + shift) % size) * groups + d))
                elif rest and d ^ 1 < groups:
                    route.append((here, here - d + (d ^ 1)))
    return held_inside(lax.ppermute(block, names, route))


def pick_kernel(order, acts, current, kept, slots, sems):
    number = pltpu.make_async_copy(order, kept, sems.at[0])
    blocks = pltpu.make_async_copy(acts.at[0], slots, sems.at[1])
    number.start()
    blocks.start()
    number.wait()
    blocks.wait()
    current[...] = slots[kept[0, 0]]


def weights_kernel(w_in, w_out, in_inside, out_inside, sems):
    copies = []
    pieces = 4
    step = w_in.shape[1] // pieces
    for i in range(pieces):
        rows = pl.ds(i * step, step)
        copies.append(pltpu.make_async_copy(w_in.at[0, rows], in_inside.at[rows], sems.at[i]))
    copies.append(pltpu.make_async_copy(w_out.at[0], out_inside, sems.at[pieces]))
    for copy in copies:
        copy.start()
    for copy in copies:
        copy.wait()


def other_kernel(order, slots, fresh, other, entering, sem):
    copy = pltpu.make_async_copy(fresh, entering, sem)
    copy.start()
    copy.wait()
    again = jnp.logical_and(lax.axis_index("section") == 0, order[0, 0] == order[0, 1])
    other[...] = jnp.where(again, entering[0], slots[order[0, 1]])


def normed(rows, gain, bias):
    values = rows.astype(F32)
    centred = values - jnp.mean(values, axis=-1, keepdims=True)
    spread = jnp.mean(centred * centred, axis=-1, keepdims=True)
    return (centred * lax.rsqrt(spread + 1e-06) * gain + bias).astype(BF16)


def project(rows, weights, *targets, width=1024):
    for start in range(0, weights.shape[1], width):
        columns = slice(start, min(start + width, weights.shape[1]))
        value = jnp.dot(rows, weights[:, columns], preferred_element_type=F32).astype(BF16)
        at = 0
        for target in targets:
            target[:, columns] = value[at : at + target.shape[0]]
            at += target.shape[0]


def attend(q, blocks, rows, mixed):
    heads = q.shape[1] // (3 * HD)
    ones = jnp.ones((sum(b.shape[0] for b in blocks), HD), BF16)
    for head in range(heads):
        at = [slice((head * 3 + j) * HD, (head * 3 + j + 1) * HD) for j in range(3)]
        query = q[rows, at[0]]
        keys = jnp.concatenate([b[:, at[1]] for b in blocks], axis=0)
        values = jnp.concatenate([b[:, at[2]] for b in blocks], axis=0)
        scores = lax.dot_general(query, keys, (((1,), (1,)), ((), ())), preferred_element_type=F32)
        powers = jnp.exp((scores - jnp.max(scores, axis=-1, keepdims=True)) * (1.0 / HD**0.5)).astype(BF16)
        out = jnp.dot(powers, jnp.concatenate([values, ones], axis=1), preferred_element_type=F32)
        mixed[rows, head * HD : (head + 1) * HD] = (out[:, :HD] / out[:, HD:]).astype(BF16)


def own_qkv_kernel(parts, *refs):
    chunks, (gain, bias, weights, qkv, hidden) = refs[:parts], refs[parts:]
    at = 0
    for chunk in chunks:
        rows = chunk.shape[0]
        hidden[at : at + rows] = normed(chunk[...], gain[...], bias[...])
        at += rows
    project(hidden[...], weights, qkv)


def others_kernel(parts, pieces, spare, *refs):
    chunks, alone, refs = refs[:parts], refs[parts : parts + spare], refs[:parts] + refs[parts + spare :]
    first = lax.axis_index("section") == 0
    gain, bias, w_in, w_out, mine = refs[parts : parts + 5]
    qkv = refs[parts + 5]
    outs = refs[parts + 6 : parts + 6 + pieces]
    hidden, mixed = refs[parts + 6 + pieces :]
    at = 0
    for chunk in chunks:
        rows = chunk.shape[0]
        value = chunk[...]
        if alone:
            start = at % alone[0].shape[0]
            value = jnp.where(first, alone[at // alone[0].shape[0]][start : start + rows], value)
        hidden[at : at + rows] = normed(value, gain[...], bias[...])
        at += rows
    project(hidden[...], w_in, qkv)
    attend(qkv, (mine, qkv), slice(0, at), mixed)
    project(mixed[...], w_out, *outs)


def own_kernel(mine, theirs, w_out, out, mixed):
    attend(mine, (mine, theirs), slice(0, mine.shape[0]), mixed)
    project(mixed[...], w_out, out)


def combine_kernel(start, *refs):
    current, own, got, result = refs[0], refs[1], refs[2:-1], refs[-1]
    rows = slice(start, start + result.shape[0])
    total = own[rows].astype(F32)
    for piece in got:
        total = total + piece[...].astype(F32)
    result[...] = (current[...].astype(F32) + total).astype(BF16)


def next_kernel(start, order, arriving, other, following):
    first = lax.axis_index("section") == 0
    take = jnp.logical_and(order[0, 0] == order[0, 1], jnp.logical_not(first))
    rows = slice(start, start + following.shape[0])
    following[...] = jnp.where(take, arriving[...], other[rows])


def held_kernel(order, slots, entering, *refs):
    arrived, held, sems = refs[:-2], refs[-2], refs[-1]
    first = lax.axis_index("section") == 0
    later = jnp.logical_not(first)

    def write(condition, slot, blocks):
        @pl.when(condition)
        def _():
            copies = []
            at = 0
            for i, block in enumerate(blocks):
                target = held.at[0, slot, pl.ds(at, block.shape[0])]
                copies.append(pltpu.make_async_copy(block, target, sems.at[i]))
                at += block.shape[0]
            for copy in copies:
                copy.start()
            for copy in copies:
                copy.wait()

    for slot in range(slots.shape[0]):
        old, new = order[0, 0] == slot, order[0, 1] == slot
        stays = jnp.logical_not(new)
        write(jnp.logical_and(first, new), slot, [entering.at[1]])
        write(jnp.logical_and(first, jnp.logical_and(stays, old)), slot, [entering.at[0]])
        write(jnp.logical_and(later, jnp.logical_and(stays, old)), slot, arrived)
        write(jnp.logical_and(stays, jnp.logical_not(old)), slot, [slots.at[slot]])


def put_kernel(tick, parts, *refs):
    chunks, out, sems = refs[:parts], refs[-2], refs[-1]
    copies = []
    at = 0
    for i, chunk in enumerate(chunks):
        rows = pl.ds(at, chunk.shape[0])
        copies.append(pltpu.make_async_copy(chunk, out.at[tick, 0, rows], sems.at[i]))
        at += chunk.shape[0]
    for copy in copies:
        copy.start()
    for copy in copies:
        copy.wait()


def last_kernel(pieces, order, *refs):
    chunks, out, sems = refs[: len(pieces)], refs[-2], refs[-1]

    @pl.when(lax.axis_index("section") > 0)
    def _():
        copies = []
        for i, (chunk, (start, size)) in enumerate(zip(chunks, pieces)):
            target = out.at[0, order[0, 1], pl.ds(start, size)]
            copies.append(pltpu.make_async_copy(chunk, target, sems.at[i]))
        for copy in copies:
            copy.start()
        for copy in copies:
            copy.wait()


def cuts(rows, shares):
    units = rows // 16
    edges = [units * sum(shares[:i]) // sum(shares) * 16 for i in range(len(shares))] + [rows]
    return [(a, b - a) for a, b in zip(edges, edges[1:]) if b > a]


def layer(pieces, chunks, got, gain, bias, w_in, w_out, alone=()):
    size = lax.axis_size("tensor")
    sections = range(lax.axis_size("section"))
    parts = len(chunks)
    rows = sum(c.shape[0] for c in chunks)
    wide, deep = w_in.shape[1], w_out.shape[0]
    width = w_in.shape[0]
    mine = call(
        functools.partial(own_qkv_kernel, parts),
        inner((rows, wide)),
        VMEM,
        [VMEM] * (parts + 3),
        [*chunks, gain, bias, w_in],
        flops=2 * rows * width * wide,
        scratch=[inner((rows, width))],
    )
    far = (size - 1) * rows
    count = (size - 1) * len(pieces)
    theirs, *sends = call(
        functools.partial(others_kernel, len(got), count, len(alone)),
        [inner((far, wide))] + [inner((n, width)) for _ in range(size - 1) for _, n in pieces],
        [VMEM] * (count + 1),
        [VMEM] * (len(got) + len(alone) + 5),
        [*got, *alone, gain, bias, w_in, w_out, mine],
        flops=2 * far * width * wide,
        scratch=[inner((far, width)), inner((far, deep))],
    )
    returned = []
    for i in range(len(pieces)):
        parts_of_i = [rotate(sends[(j - 1) * len(pieces) + i], -j, sections) for j in range(1, size)]
        returned.append(parts_of_i)
    own = call(
        own_kernel,
        inner((rows, width)),
        VMEM,
        [VMEM] * 3,
        [mine, theirs, w_out],
        flops=2 * rows * width * deep,
        scratch=[inner((rows, deep))],
    )
    return own, returned


def body(acts, fresh, order, ln_gain, ln_bias, wqkv, wo):
    rows, width = acts.shape[2:]
    ticks = fresh.shape[0]
    dma = pltpu.SemaphoreType.DMA
    acts, fresh, order, wqkv, wo = map(outside, (acts, fresh, order, wqkv, wo))
    current, order, slots = call(
        pick_kernel,
        [inner((rows, width)), pltpu.SMEM(order.shape, order.dtype), inner(acts.shape[1:])],
        [VMEM, SMEM, VMEM],
        [ANY, ANY],
        [order, acts],
        scratch=[dma((2,))],
    )
    other, entering = call(
        other_kernel,
        [inner((rows, width)), inner(fresh.shape)],
        [VMEM, VMEM],
        [SMEM, VMEM, ANY],
        [order, slots, fresh],
        scratch=[dma],
    )
    w_in, w_out = call(
        weights_kernel,
        [inner(wqkv.shape[1:]), inner(wo.shape[1:])],
        [VMEM, VMEM],
        [ANY, ANY],
        [wqkv, wo],
        scratch=[dma((5,))],
        limit=24,
        flops=1 << 30,
    )
    shifts = range(1, lax.axis_size("tensor"))
    sections = range(lax.axis_size("section"))
    chunks = [current]
    got = [rotate(current, j, sections) for j in shifts]
    alone = [rotate(other, j, [0]) for j in shifts]
    section_out = held = None
    for tick in range(ticks):
        here_at = [sum(c.shape[0] for c in chunks[:i]) for i in range(len(chunks))]
        if tick:
            before, parts = arrived, len(arrived)
        pieces = cuts(rows, SHARES[tick])
        own, returned = layer(pieces, chunks, got, ln_gain, ln_bias, w_in, w_out, alone if tick else ())
        ready = []
        if tick:
            section_out = call(
                functools.partial(put_kernel, 0, parts),
                pltpu.HBM((ticks, 1, rows, width), BF16),
                ANY,
                [VMEM] * parts,
                results,
                scratch=[dma((parts,))],
                wait=[own],
            )
            held = call(
                held_kernel,
                pltpu.HBM(acts.shape, BF16),
                ANY,
                [SMEM, VMEM, VMEM] + [VMEM] * parts,
                [order, slots, entering, *before],
                scratch=[dma((parts,))],
                wait=[own],
            )
            section_out, held = outside(section_out), outside(held)
            ready = [section_out, held]
        results, arrived = [], []
        for i, (start, size) in enumerate(pieces):

            holder = max(k for k, at in enumerate(here_at) if at <= start)

            def combine(*refs, start=start, size=size, at=here_at[holder]):
                combine_kernel(start, refs[0].at[pl.ds(start - at, size)], *refs[1:])

            result = call(
                combine,
                inner((size, width)),
                VMEM,
                [VMEM] * (2 + len(returned[i])),
                [chunks[holder], own, *returned[i]],
                wait=ready,
            )
            results.append(result)
            arrived.append(held_inside(from_behind(result, "section", RING[tick])))
        if tick == 0:
            chunks, swapped = [], []
            for i, (start, size) in enumerate(pieces):
                chunks.append(
                    call(
                        functools.partial(next_kernel, start),
                        inner((size, width)),
                        VMEM,
                        [SMEM, VMEM, VMEM],
                        [order, arrived[i], other],
                    )
                )
                swapped.append([rotate(chunks[i], j, sections[1:], rest=True) for j in shifts])
            got = [block for of_j in zip(*swapped) for block in of_j]
    parts = len(pieces)
    section_out = call(
        functools.partial(put_kernel, ticks - 1, parts),
        pltpu.HBM((ticks, 1, rows, width), BF16),
        ANY,
        [VMEM] * parts + [ANY],
        [*results, section_out],
        scratch=[dma((parts,))],
        aliases={parts: 0},
    )
    for which in (range(parts - 1), range(parts - 1, parts)):
        held = call(
            functools.partial(last_kernel, [pieces[i] for i in which]),
            pltpu.HBM(acts.shape, BF16),
            ANY,
            [SMEM] + [VMEM] * len(which) + [ANY],
            [order, *(arrived[i] for i in which), outside(held)],
            scratch=[dma((len(which),))],
            aliases={len(which) + 1: 0},
        )
    return section_out, held


def solution(mesh):
    return jax.shard_map(
        body,
        mesh=mesh,
        in_specs=(
            P("section", "dp", "tensor", None),
            P("dp", "tensor", None),
            P("section", None),
            P("section", None),
            P("section", None),
            P("section", None, "tensor"),
            P("section", "tensor", None),
        ),
        out_specs=(P("dp", "section", "tensor", None), P("section", "dp", "tensor", None)),
        check_vma=False,
    )
```
